32 devices in a mesh: gx: 4 (over y, core), gy: 4 (over z), gz: 2 (over x).
Axes of the slice: x: 2, y: 2, z: 4, core: 2. Of those that a mesh axis runs over, the one named last changes fastest.
Arguments:
- permittivity: float32 [32, 128, 256], P('gx', 'gy', 'gz'), may hold values from 1 to 9
- loss: float32 [32, 128, 256], P('gx', 'gy', 'gz'), may hold values from 0 to 0.2
- fwd_electric: float32 [3, 32, 128, 256], P(None, 'gx', 'gy', 'gz'), may hold values from -6 to 6
- fwd_magnetic: float32 [3, 32, 128, 256], P(None, 'gx', 'gy', 'gz'), may hold values from -6 to 6
- adj_electric: float32 [3, 32, 128, 256], P(None, 'gx', 'gy', 'gz'), may hold values from -200 to 200
- adj_magnetic: float32 [3, 32, 128, 256], P(None, 'gx', 'gy', 'gz'), may hold values from -200 to 200
- wavelet: float32 [64], replicated, may hold values from -6 to 6
- residuals: float32 [256, 64], P(('gx', 'gy', 'gz')), may hold values from -24 to 24
- source_cell: int32 [1], replicated, may hold values from 0 to 1048575
- receiver_cells: int32 [256], replicated, may hold values from 0 to 1048575
- start_step: int32 [1], replicated, may hold values from 0 to 60
Outputs:
- direction: float32 [32, 128, 256], P('gx', 'gy', 'gz')
- grad_rms: float32 [], replicated
The draws below stay inside these ranges and needn't reach their ends.
Inputs may be any that keep to these rules, and one draw needn't show every extreme that they name: source_cell[0] is a flat index of a cell. receiver_cells[r] is the flat index of receiver r's cell; several receivers may share a cell. Samples start_step to start_step + 3 exist in every trace.
All inputs are finite; a program needn't handle non-finite values.
Results may differ from the reference program's by a relative error of at most 0.0003.
Values sent between devices are 32-bit elements; how exact they have to be, the bound alone decides.
A program may use at most 128 MiB of HBM per device.

```python
import math
import jax
import jax.numpy as jnp
from jax import lax

STEPS = 4
TRACE = 64
NREC = 256
NX = 32
NY = 128
NZ = 256


def adjoint_field(key):
    keys = jax.random.split(key, 4)
    ramp = 3.0 ** (jnp.arange(NX, dtype=jnp.float32) / NX)
    scale_x = ramp
    scale_y = jnp.exp(jax.random.uniform(keys[2], (NY,), jnp.float32, 0.0, math.log(4.0)))
    scale_z = jnp.exp(jax.random.uniform(keys[3], (NZ,), jnp.float32, 0.0, math.log(2.0)))
    base = jnp.clip(jax.random.normal(keys[0], (3, NX, NY, NZ), jnp.float32), -6.0, 6.0)
    return base * scale_x[None, :, None, None] * scale_y[None, None, :, None] * scale_z[None, None, None, :]


def draw_adj_electric(key, part):
    return adjoint_field(jax.random.fold_in(key, 11))


def draw_adj_magnetic(key, part):
    return adjoint_field(jax.random.fold_in(key, 23))


def place_ends(values, rng, low, high):
    longest = values.shape.index(max(values.shape))
    spots = []
    for shift in (0, 1):
        where = [jax.random.randint(jax.random.fold_in(rng, axis), (), 0, length) for axis, length in enumerate(values.shape)]
        where[longest] = (where[longest] + shift) % values.shape[longest]
        spots.append(tuple(where))
    return values.at[spots[0]].set(low).at[spots[1]].set(high)


def levels(stream_key, shape, cuts, low, largest):
    def one(dim, parts):
        steps = jax.random.uniform(jax.random.fold_in(jax.random.fold_in(stream_key, 6), dim), (parts,), jnp.float32, low / len(cuts), largest / len(cuts))
        return jnp.repeat(jnp.exp(steps), shape[dim] // parts).reshape((-1,) + (1,) * (len(shape) - dim - 1))

    gain = one(*cuts[0])
    for cut in cuts[1:]:
        gain = gain * one(*cut)
    return gain


def normal_values(stream_key, dims, spread, limit, shards=(), kind=jnp.bfloat16):
    values = spread * jax.random.normal(stream_key, dims, jnp.float32)
    if shards:
        values = values * levels(stream_key, dims, shards, -0.22, 0.18)
    return jnp.clip(values, -limit, limit).astype(kind)


def setup_inputs(seed: int = 0) -> dict:
    seeds = jax.random.split(jax.random.key(seed), 12)
    return {
        "permittivity": jnp.clip(jnp.exp(math.log(9.0) - 2.1972246 * jax.random.uniform(seeds[0], (NX, NY, NZ), jnp.float32) ** levels(seeds[0], (NX, NY, NZ), ((0, 4), (1, 4), (2, 2)), -0.2, 0.2)), 1.0, 9.0),
        "loss": jnp.clip(0.2 * jax.random.uniform(seeds[1], (NX, NY, NZ), jnp.float32) ** levels(seeds[1], (NX, NY, NZ), ((0, 4), (1, 4), (2, 2)), -0.2, 0.2), 0.0, 0.2),
        "fwd_electric": normal_values(seeds[2], (3, NX, NY, NZ), 1.0, 6.0, ((1, 4), (2, 4), (3, 2)), jnp.float32),
        "fwd_magnetic": normal_values(seeds[3], (3, NX, NY, NZ), 1.0, 6.0, ((1, 4), (2, 4), (3, 2)), jnp.float32),
        "adj_electric": draw_adj_electric(jax.random.fold_in(seeds[11], 71), 0),
        "adj_magnetic": draw_adj_magnetic(jax.random.fold_in(seeds[11], 71), 0),
        "wavelet": normal_values(seeds[6], (TRACE,), 1.0, 6.0, (), jnp.float32),
        "residuals": normal_values(seeds[7], (NREC, TRACE), 4.0, 24.0, ((0, 32),), jnp.float32),
        "source_cell": jax.random.randint(seeds[8], (1,), 0, NX * NY * NZ).astype(jnp.int32),
        "receiver_cells": place_ends(jax.random.randint(seeds[9], (NREC,), 0, NX * NY * NZ), jax.random.fold_in(seeds[9], 1), 0, (NX * NY * NZ) - 1).astype(jnp.int32),
        "start_step": jax.random.randint(seeds[10], (1,), 0, TRACE - STEPS + 1).astype(jnp.int32),
    }


def shifted_above(field, axis):
    rest = lax.slice_in_dim(field, 1, field.shape[axis], axis=axis)
    edge = jnp.zeros_like(lax.slice_in_dim(field, 0, 1, axis=axis))
    return jnp.concatenate([rest, edge], axis)

def shifted_below(field, axis):
    rest = lax.slice_in_dim(field, 0, field.shape[axis] - 1, axis=axis)
    edge = jnp.zeros_like(lax.slice_in_dim(field, 0, 1, axis=axis))
    return jnp.concatenate([edge, rest], axis)

def yee_step(electric, magnetic, keep, curl):
    electric_x, electric_y, electric_z = electric
    magnetic_x, magnetic_y, magnetic_z = magnetic
    magnetic_x = magnetic_x - 0.5 * (shifted_above(electric_z, 1) - electric_z - (shifted_above(electric_y, 2) - electric_y))
    magnetic_y = magnetic_y - 0.5 * (shifted_above(electric_x, 2) - electric_x - (shifted_above(electric_z, 0) - electric_z))
    magnetic_z = magnetic_z - 0.5 * (shifted_above(electric_y, 0) - electric_y - (shifted_above(electric_x, 1) - electric_x))
    electric_x = keep * electric_x + curl * (magnetic_z - shifted_below(magnetic_z, 1) - (magnetic_y - shifted_below(magnetic_y, 2)))
    electric_y = keep * electric_y + curl * (magnetic_x - shifted_below(magnetic_x, 2) - (magnetic_z - shifted_below(magnetic_z, 0)))
    electric_z = keep * electric_z + curl * (magnetic_y - shifted_below(magnetic_y, 0) - (magnetic_x - shifted_below(magnetic_x, 1)))
    return ((electric_x, electric_y, electric_z), (magnetic_x, magnetic_y, magnetic_z))

def split_index(flat):
    first = flat // (NY * NZ)
    second = flat // NZ % NY
    third = flat % NZ
    return (first, second, third)

def reference(permittivity, loss, fwd_electric, fwd_magnetic, adj_electric, adj_magnetic, wavelet, residuals, source_cell, receiver_cells, start_step):
    keep = (1.0 - loss) / (1.0 + loss)
    curl = 0.5 / (permittivity * (1.0 + loss))
    start = start_step[0]
    zero_index = jnp.zeros((), jnp.int32)
    src_i, src_j, src_k = split_index(source_cell[0])
    rec_i, rec_j, rec_k = split_index(receiver_cells)
    electric = (fwd_electric[0], fwd_electric[1], fwd_electric[2])
    magnetic = (fwd_magnetic[0], fwd_magnetic[1], fwd_magnetic[2])
    snapshots = [electric]
    for index in range(STEPS):
        electric, magnetic = yee_step(electric, magnetic, keep, curl)
        sample = lax.dynamic_slice_in_dim(wavelet, start + index, 1)[0]
        electric = (electric[0], electric[1], electric[2].at[src_i, src_j, src_k].add(sample))
        snapshots.append(electric)
    window = lax.dynamic_slice(residuals, (zero_index, start), (residuals.shape[0], STEPS))
    adjoint = (adj_electric[0], adj_electric[1], adj_electric[2])
    adjoint_mag = (adj_magnetic[0], adj_magnetic[1], adj_magnetic[2])
    gradient = jnp.zeros(permittivity.shape, jnp.float32)
    for index in range(STEPS):
        adjoint, adjoint_mag = yee_step(adjoint, adjoint_mag, keep, curl)
        adjoint = (adjoint[0], adjoint[1], adjoint[2].at[rec_i, rec_j, rec_k].add(window[:, STEPS - 1 - index]))
        later = STEPS - index
        change = [snapshots[later][c] - snapshots[later - 1][c] for c in range(3)]
        gradient = gradient + (change[0] * adjoint[0] + change[1] * adjoint[1] + change[2] * adjoint[2])
    gradient = -gradient / permittivity
    grad_rms = jnp.sqrt(jnp.sum(gradient * gradient) / (NX * NY * NZ) + 1e-06)
    return (gradient / grad_rms, grad_rms)
```

```python
import functools

import jax
import jax.numpy as jnp
from jax import lax
from jax.experimental import pallas as pl
from jax.experimental.pallas import tpu as pltpu
from jax.sharding import PartitionSpec as P

STEPS = 4
MESH = pl.DeviceIdType.MESH
F32 = jnp.float32
HALF = 0.5


def kernel(
    sizes,
    wav_hbm,
    src_hbm,
    start_hbm,
    cells_hbm,
    perm_hbm,
    loss_hbm,
    fe_hbm,
    fm_hbm,
    ae_hbm,
    am_hbm,
    res_hbm,
    out_ref,
    rms_ref,
    E,
    H,
    perm,
    loss,
    keep,
    curl,
    D,
    A,
    inj,
    R_all,
    grad,
    HP,
    xU,
    xD,
    ysU,
    ysD,
    yU,
    yD,
    zsU,
    zsD,
    zU,
    zD,
    zX,
    zXU,
    e1s,
    e2s,
    e1r,
    e2r,
    hys,
    hyr,
    hzs,
    part,
    sums,
    wav_ref,
    src_ref,
    start_ref,
    cells_ref,
    res_ref,
    mine,
    load_sem,
    f_send,
    f_recv,
    h_send,
    h_recv,
    g_send,
    g_recv,
    r_send,
    r_recv,
):
    gx, gy, gz = sizes
    nx, ny, nz = perm.shape
    pad = H.shape[3] - ny
    O = slice(pad, pad + ny)
    R = slice(0, pad + ny)
    above = slice(pad + 1, pad + ny + 1)
    ix, iy, iz = lax.axis_index("gx"), lax.axis_index("gy"), lax.axis_index("gz")
    nplane = gy * gz
    plane = iy * gz + iz

    loads = [
        pltpu.make_async_copy(fe_hbm, E.at[0, :, :, O, :], load_sem.at[0]),
        pltpu.make_async_copy(ae_hbm, E.at[1, :, :, O, :], load_sem.at[1]),
        pltpu.make_async_copy(fm_hbm, H.at[0, :, 1 : nx + 1, O, :], load_sem.at[2]),
        pltpu.make_async_copy(am_hbm, H.at[1, :, 1 : nx + 1, O, :], load_sem.at[3]),
        pltpu.make_async_copy(loss_hbm, loss, load_sem.at[4]),
        pltpu.make_async_copy(perm_hbm, perm, load_sem.at[5]),
    ]
    small = [
        pltpu.make_async_copy(start_hbm, start_ref, load_sem.at[6]),
        pltpu.make_async_copy(res_hbm, res_ref, load_sem.at[7]),
        pltpu.make_async_copy(src_hbm, src_ref, load_sem.at[8]),
        pltpu.make_async_copy(wav_hbm, wav_ref, load_sem.at[9]),
        pltpu.make_async_copy(cells_hbm, cells_ref, load_sem.at[10]),
    ]
    loads = loads + small
    for load in small:
        load.start()
    loads, small = loads[:6], loads[6:]
    for load in loads:
        load.start()

    total_devices = gx * nplane
    me = ix * nplane + plane
    peers = []
    for d in range(1, total_devices):
        q = lax.rem(me + d, total_devices)
        peers.append((q, (q // nplane, lax.rem(q // gz, gy), lax.rem(q, gz))))

    zero_plane = jnp.zeros((ny, nz), F32)
    zero_tile = jnp.zeros((pad, nz), F32)
    for s in range(2):
        for c in range(3):
            H[s, c, 0, O, :] = zero_plane
            for p in range(nx):
                E[s, c, p, 0:pad, :] = zero_tile
                E[s, c, p, pad + ny : pad + ny + pad, :] = zero_tile
                H[s, c, p + 1, 0:pad, :] = zero_tile
    for buffer in (HP, xU, xD, yU, yD, zU, zD, zX, zXU, e1r, e2r, hyr):
        buffer[...] = jnp.zeros(buffer.shape, F32)

    barrier = pltpu.get_barrier_semaphore()
    for _, dev in peers:
        pl.semaphore_signal(barrier, inc=1, device_id=dev, device_id_type=MESH)

    per, trace = res_hbm.shape
    small[0].wait()
    small[1].wait()
    begin = start_ref[0]
    time_at = lax.broadcasted_iota(jnp.int32, (trace, nz), 0)
    slot = lax.div(lax.broadcasted_iota(jnp.int32, (trace, nz), 1), per)
    pick = jnp.where(time_at == begin + STEPS - 1 - slot, 1.0, 0.0)
    wide = jnp.dot(res_ref[...], pick, precision=lax.Precision.HIGHEST, preferred_element_type=F32)
    own = lax.rem(lax.broadcasted_iota(jnp.int32, (per, nz), 1), per)
    own = own == lax.broadcasted_iota(jnp.int32, (per, nz), 0)
    mine[0] = jnp.sum(jnp.where(own, wide, 0.0), axis=0, keepdims=True)
    R_all[pl.ds(me, 1)] = mine[...]
    for load in small[2:]:
        load.wait()
    pl.semaphore_wait(barrier, len(peers))

    def remote(src, dst, ssem, rsem, dev):
        return pltpu.make_async_remote_copy(
            src_ref=src, dst_ref=dst, send_sem=ssem, recv_sem=rsem,
            device_id=dev, device_id_type=MESH,
        )

    def exchange(src, slots, send_sems, recv_sems):
        copies = []
        for d, (q, dev) in enumerate(peers):
            send = remote(src, slots.at[me], send_sems.at[d], recv_sems.at[me], dev)
            recv = remote(src, slots.at[q], send_sems.at[d], recv_sems.at[q], dev)
            send.start()
            copies.append((send, recv))
        return copies

    def settle(copies):
        for send, recv in copies:
            recv.wait_recv()
        for send, recv in copies:
            send.wait_send()

    has = {
        "+x": ix < gx - 1, "-x": ix > 0, "+y": iy < gy - 1,
        "-y": iy > 0, "+z": iz < gz - 1, "-z": iz > 0,
    }
    flip = {"+": "-", "-": "+"}

    def route(steps):
        dev = [ix, iy, iz]
        size = (gx, gy, gz)
        can_send, can_recv = True, True
        for step in steps:
            axis = "xyz".index(step[1])
            dev[axis] = jnp.clip(dev[axis] + (1 if step[0] == "+" else -1), 0, size[axis] - 1)
            back = flip[step[0]] + step[1]
            can_send = has[step] if can_send is True else can_send & has[step]
            can_recv = has[back] if can_recv is True else can_recv & has[back]
        return tuple(dev), can_send, can_recv

    def face(s, slot, d):
        table = (
            (("+x",), E.at[s, :, nx - 1, O, :], xU.at[slot, s, :, O, :]),
            (("-x",), E.at[s, 1:3, 0, O, :], xD.at[slot, s, :, O, :]),
            (("+y",), ysU.at[s], yU.at[slot, s]),
            (("-y",), ysD.at[s], yD.at[slot, s]),
            (("+z",), zsU.at[s], zU.at[slot, s, 0:ny, :]),
            (("-z",), zsD.at[s], zD.at[slot, s, O, :]),
            (("+x", "-y"), e1s.at[s], e1r.at[slot, s]),
            (("-x", "+y"), e2s.at[s], e2r.at[slot, s]),
            (("+x", "-z"), zsD.at[s], zX.at[slot, s]),
            (("-x", "+z"), zsU.at[s], zXU.at[slot, s]),
            (("+y", "-z"), zsD.at[s, ny - pad : ny, :], zD.at[slot, s, 0:pad, :]),
            (("-y", "+z"), zsU.at[s, 0:pad, :], zU.at[slot, s, ny : ny + pad, :]),
        )
        steps, source, target = table[d]
        dev, can_send, can_recv = route(steps)
        return remote(source, target, f_send.at[s, d], f_recv.at[slot, s, d], dev), can_send, can_recv

    def first(s, d):
        table = (
            (("+x",), H.at[s, 1:3, nx, O, :], H.at[s, 1:3, 0, O, :]),
            (("+y",), hys.at[s], hyr.at[s]),
            (("+z",), hzs.at[s], HP.at[s]),
        )
        steps, source, target = table[d]
        dev, can_send, can_recv = route(steps)
        return remote(source, target, h_send.at[s, d], h_recv.at[s, d], dev), can_send, can_recv

    def start(item):
        copy, can_send, _ = item

        @pl.when(can_send)
        def _():
            copy.start()

    def finish(item):
        copy, can_send, _ = item

        @pl.when(can_send)
        def _():
            copy.wait_send()

    def arrive(item):
        copy, _, can_recv = item

        @pl.when(can_recv)
        def _():
            copy.wait_recv()

    lane = lax.broadcasted_iota(jnp.int32, (ny, nz), 1)
    row = lax.broadcasted_iota(jnp.int32, (ny, nz), 0)

    def pack_column(acc, value, source, j):
        return jnp.where(lane == j, pltpu.roll(value, (j - source) % nz, 1), acc)

    def down_z(value, halo, j):
        rolled = pltpu.roll(value, 1, 1)
        return jnp.where(lane == 0, pltpu.roll(halo, (nz - j) % nz, 1), rolled)

    def pack_rows(s):
        for p in range(nx):
            for c in range(3):
                ysU[s, c, p : p + 1, :] = E[s, c, p, pad + ny - 1 : pad + ny, :]
            ysD[s, 0, p : p + 1, :] = E[s, 0, p, pad : pad + 1, :]
            ysD[s, 1, p : p + 1, :] = E[s, 2, p, pad : pad + 1, :]
        e1s[s] = E[s, 0, nx - 1, pad : pad + 1, :]
        e2s[s] = E[s, 1, 0, pad + ny - 1 : pad + ny, :]

    def pack_low(s):
        @pl.when(has["-z"])
        def _():
            acc = jnp.zeros((ny, nz), F32)
            for p in range(nx):
                acc = pack_column(acc, E[s, 0, p, O, :], 0, p)
                acc = pack_column(acc, E[s, 1, p, O, :], 0, nx + p)
            zsD[s] = acc

    def pack_high(s):
        @pl.when(has["+z"])
        def _():
            acc = jnp.zeros((ny, nz), F32)
            for p in range(nx):
                acc = pack_column(acc, E[s, 0, p, O, :], nz - 1, p)
                acc = pack_column(acc, E[s, 1, p, O, :], nz - 1, nx + p)
                acc = pack_column(acc, E[s, 2, p, O, :], nz - 1, 2 * nx + p)
            zsU[s] = acc

    def send_rest(s, slot):
        pack_rows(s)
        for d in (6, 7, 2, 3):
            start(face(s, slot, d))
        pack_low(s)
        pack_high(s)
        for d in (8, 9, 10, 11, 4, 5):
            start(face(s, slot, d))

    def send_magnetic(s):
        start(first(s, 0))
        for p in range(nx):
            hys[s, 0, p : p + 1, :] = H[s, 0, p + 1, pad + ny - 1 : pad + ny, :]
            hys[s, 1, p : p + 1, :] = H[s, 2, p + 1, pad + ny - 1 : pad + ny, :]
        start(first(s, 1))

        @pl.when(has["+z"])
        def _():
            acc = jnp.zeros((ny, nz), F32)
            for p in range(nx):
                acc = pack_column(acc, H[s, 1, p + 1, O, :], nz - 1, p)
                acc = pack_column(acc, H[s, 0, p + 1, O, :], nz - 1, nx + p)
            hzs[s] = acc

        start(first(s, 2))

    half_x = jnp.where(has["-x"], HALF, 0.0)
    half_rows = jnp.where(lax.broadcasted_iota(jnp.int32, (pad + ny, nz), 0) < pad, jnp.where(has["-y"], HALF, 0.0), HALF)
    lane_r = lax.broadcasted_iota(jnp.int32, (pad + ny, nz), 1)

    def up_z(value, halo, j):
        edge = lane_r[: value.shape[0]] == nz - 1
        return jnp.where(edge, pltpu.roll(halo, (nz - 1 - j) % nz, 1), pltpu.roll(value, nz - 1, 1))

    def update_h(s, slot, opening):
        for d in (2, 3, 5, 10):
            arrive(face(s, slot, d))
        if opening:
            arrive(first(s, 1))
            for p in range(nx):
                H[s, 0, p + 1, pad - 1 : pad, :] = hyr[s, 0, p : p + 1, :]
                H[s, 2, p + 1, pad - 1 : pad, :] = hyr[s, 1, p : p + 1, :]
        for p in range(nx):
            for c in range(3):
                E[s, c, p, pad - 1 : pad, :] = yU[slot, s, c, p : p + 1, :]
            E[s, 0, p, pad + ny : pad + ny + 1, :] = yD[slot, s, 0, p : p + 1, :]
            E[s, 2, p, pad + ny : pad + ny + 1, :] = yD[slot, s, 1, p : p + 1, :]
        halo = zD[slot, s]
        up = slice(1, pad + ny + 1)
        for p in range(nx):
            if p == nx - 1:
                for d in (0, 1, 6, 7, 8):
                    arrive(face(s, slot, d))
                xU[slot, s, 0, pad + ny : pad + ny + 1, :] = e1r[slot, s]
                xD[slot, s, 0, pad - 1 : pad, :] = e2r[slot, s]
                next_y, next_z = xD[slot, s, 0, R, :], xD[slot, s, 1, O, :]
            else:
                next_y, next_z = E[s, 1, p + 1, R, :], E[s, 2, p + 1, O, :]
            ex, ey, ez = E[s, 0, p, R, :], E[s, 1, p, R, :], E[s, 2, p, R, :]
            hx = H[s, 0, p + 1, R, :] - half_rows * (E[s, 2, p, up, :] - ez - (up_z(ey, halo, nx + p) - ey))
            hy = H[s, 1, p + 1, O, :] - HALF * (up_z(ex[pad:], halo[pad:], p) - ex[pad:] - (next_z - ez[pad:]))
            hz = H[s, 2, p + 1, R, :] - half_rows * (next_y - ey - (E[s, 0, p, up, :] - ex))
            H[s, 0, p + 1, R, :] = hx
            H[s, 1, p + 1, O, :] = hy
            H[s, 2, p + 1, R, :] = hz
        if opening:
            arrive(first(s, 0))
        ex, ey, ez = xU[slot, s, 0, O, :], xU[slot, s, 1, O, :], xU[slot, s, 2, O, :]
        side = H[s, 1, 0, O, :] - half_x * (up_z(ex, zX[slot, s], nx - 1) - ex - (E[s, 2, 0, O, :] - ez))
        H[s, 1, 0, O, :] = side
        side = H[s, 2, 0, O, :] - half_x * (E[s, 1, 0, O, :] - ey - (xU[slot, s, 0, above, :] - ex))
        H[s, 2, 0, O, :] = side
        for d in (4, 9, 11):
            arrive(face(s, slot, d))
        if opening:
            arrive(first(s, 2))

        @pl.when(has["-z"])
        def _():
            below = zU[slot, s, 0:ny, :]
            wide = jnp.where(lane == 3 * nx, pltpu.roll(zXU[slot, s], nx, 1), below)
            along = pltpu.roll(pltpu.roll(wide, nz - 1, 1) - wide, nz - 2 * nx, 1)
            across = pltpu.roll(zU[slot, s, 1 : ny + 1, :] - below, nz - nx, 1)
            turn = jnp.where(lane < nx, along, across)
            HP[s] = HP[s] - jnp.where(lane < nx, HALF, -HALF) * (zsD[s] - below - turn)

    src = src_ref[0]
    total_z, total_y = nz * gz, ny * gy
    src_i = lax.div(src, total_y * total_z) - ix * nx
    src_j = lax.rem(lax.div(src, total_z), total_y) - iy * ny
    src_k = lax.rem(src, total_z) - iz * nz
    src_mask = (row == src_j) & (lane == src_k)

    def update_e(s, k, slot):
        for d in range(12):
            finish(face(s, slot, d))
        more = k < STEPS - 1
        halo = HP[s]
        below = slice(pad - 1, pad + ny - 1)
        pulse = wav_ref[begin + k]
        for p in (nx - 1,) + tuple(range(nx - 1)):
            hx, hy, hz = H[s, 0, p + 1, O, :], H[s, 1, p + 1, O, :], H[s, 2, p + 1, O, :]
            kp, cl = keep[p], curl[p]
            ox, oy, oz = E[s, 0, p, O, :], E[s, 1, p, O, :], E[s, 2, p, O, :]
            ex = kp * ox + cl * (hz - H[s, 2, p + 1, below, :] - (hy - down_z(hy, halo, p)))
            ey = kp * oy + cl * (hx - down_z(hx, halo, nx + p) - (hz - H[s, 2, p, O, :]))
            ez = kp * oz + cl * (hy - H[s, 1, p, O, :] - (hx - H[s, 0, p + 1, below, :]))
            if s == 0:
                ez = ez + jnp.where(src_mask, jnp.where(src_i == p, pulse, 0.0), 0.0)
                D[k, 0, p] = ex - ox
                D[k, 1, p] = ey - oy
                D[k, 2, p] = ez - oz
            else:
                ez = ez + inj[k, p * ny : (p + 1) * ny, :]
                A[k, 0, p] = ex
                A[k, 1, p] = ey
                A[k, 2, p] = ez
            E[s, 0, p, O, :] = ex
            E[s, 1, p, O, :] = ey
            E[s, 2, p, O, :] = ez
            if p == nx - 1 or p == 0:
                dx = 0 if p == nx - 1 else 1

                @pl.when(more)
                def _():
                    start(face(s, 1 - slot, dx))

        @pl.when(more)
        def _():
            send_rest(s, 1 - slot)

    def injection():
        cells = cells_ref[...]
        count = cells.shape[1]
        i = lax.div(cells, total_y * total_z) - ix * nx
        j = lax.rem(lax.div(cells, total_z), total_y) - iy * ny
        k = lax.rem(cells, total_z) - iz * nz
        inside = (i >= 0) & (i < nx) & (j >= 0) & (j < ny)
        where = jnp.where(inside, i * ny + j, -1)
        rows = lax.broadcasted_iota(jnp.int32, (nx * ny, count), 0)
        spots = jnp.where(rows == where, 1.0, 0.0).astype(jnp.bfloat16)
        depth = lax.broadcasted_iota(jnp.int32, (nz, count), 0) == k
        nt = (((1,), (1,)), ((), ()))
        spread_lane = lax.broadcasted_iota(jnp.int32, (nz, count), 0)
        spread_rec = lax.rem(lax.broadcasted_iota(jnp.int32, (nz, count), 1), per)
        holder = lax.div(lax.broadcasted_iota(jnp.int32, (total_devices, count), 1), per)
        holder = holder == lax.broadcasted_iota(jnp.int32, (total_devices, count), 0)
        packed = R_all[:, 0, :]
        for m in range(STEPS):
            spread = jnp.where(spread_lane == m * per + spread_rec, 1.0, 0.0)
            found = jnp.dot(packed, spread, precision=lax.Precision.HIGHEST, preferred_element_type=F32)
            samples = jnp.sum(jnp.where(holder, found, 0.0), axis=0, keepdims=True)
            rest = jnp.where(depth, samples, 0.0)
            total = jnp.zeros((nx * ny, nz), F32)
            for _ in range(3):
                head = rest.astype(jnp.bfloat16)
                rest = rest - head.astype(F32)
                total = total + lax.dot_general(spots, head, nt, preferred_element_type=F32)
            inj[m] = total

    for s in range(2):
        loads[s].wait()
        start(face(s, 0, 0))
        start(face(s, 0, 1))
        send_rest(s, 0)
    gather = exchange(mine.at[0], R_all, g_send, g_recv)
    for s in range(2):
        loads[2 + s].wait()
        send_magnetic(s)
    loads[4].wait()
    loads[5].wait()
    for p in range(nx):
        lo = loss[p]
        keep[p] = (1.0 - lo) / (1.0 + lo)
        curl[p] = 0.5 / (perm[p] * (1.0 + lo))

    for s in range(2):
        for d in range(3):
            finish(first(s, d))
        update_h(s, 0, True)
    update_e(0, 0, 0)
    settle(gather)
    injection()
    update_e(1, 0, 0)

    def body(k, carry):
        slot = lax.rem(k, 2)
        for s in range(2):
            update_h(s, slot, False)
            update_e(s, k, slot)
        return carry

    lax.fori_loop(1, STEPS, body, 0)

    squares = jnp.zeros((ny, nz), F32)
    for p in range(nx):
        total = jnp.zeros((ny, nz), F32)
        for m in range(STEPS):
            n = STEPS - 1 - m
            total = total + (D[n, 0, p] * A[m, 0, p] + D[n, 1, p] * A[m, 1, p] + D[n, 2, p] * A[m, 2, p])
        g = -total / perm[p]
        grad[p] = g
        squares = squares + g * g
    part[0] = jnp.sum(squares, axis=0, keepdims=True)
    sums[pl.ds(me, 1)] = part[...]
    settle(exchange(part.at[0], sums, r_send, r_recv))
    tile = sums[:, 0, :]
    total = jnp.sum(jnp.sum(tile, axis=0, keepdims=True), axis=1, keepdims=True)
    rms = jnp.sqrt(total / (nx * ny * nz * gx * gy * gz) + 1e-06)
    rms_ref[...] = rms
    inverse = 1.0 / rms
    for p in range(nx):
        out_ref[p] = grad[p] * inverse


def per_device(
    permittivity, loss, fwd_electric, fwd_magnetic, adj_electric, adj_magnetic,
    wavelet, residuals, source_cell, receiver_cells, start_step,
):
    sizes = tuple(lax.axis_size(a) for a in ("gx", "gy", "gz"))
    gx, gy, gz = sizes
    nx, ny, nz = permittivity.shape
    devices = gx * gy * gz
    count = receiver_cells.shape[0]
    vmem = pl.BlockSpec(memory_space=pltpu.VMEM)
    hbm = pl.BlockSpec(memory_space=pltpu.HBM)
    dma = pltpu.SemaphoreType.DMA
    block = (nx, ny, nz)
    tall = ny + 16
    direction, rms = pl.pallas_call(
        functools.partial(kernel, sizes),
        out_shape=(
            pltpu.VMEM(block, F32),
            jax.ShapeDtypeStruct((1, 1), F32),
        ),
        in_specs=[hbm] * 11,
        out_specs=(vmem, vmem),
        scratch_shapes=[
            pltpu.VMEM((2, 3, nx, tall, nz), F32),
            pltpu.VMEM((2, 3, nx + 1, ny + 8, nz), F32),
            pltpu.VMEM(block, F32),
            pltpu.VMEM(block, F32),
            pltpu.VMEM(block, F32),
            pltpu.VMEM(block, F32),
            pltpu.VMEM((STEPS, 3) + block, F32),
            pltpu.VMEM((STEPS, 3) + block, F32),
            pltpu.VMEM((STEPS, nx * ny, nz), F32),
            pltpu.VMEM((devices, 1, nz), F32),
            pltpu.VMEM(block, F32),
            pltpu.VMEM((2, ny, nz), F32),
            pltpu.VMEM((2, 2, 3, tall, nz), F32),
            pltpu.VMEM((2, 2, 2, tall, nz), F32),
            pltpu.VMEM((2, 3, nx, nz), F32),
            pltpu.VMEM((2, 2, nx, nz), F32),
            pltpu.VMEM((2, 2, 3, nx, nz), F32),
            pltpu.VMEM((2, 2, 2, nx, nz), F32),
            pltpu.VMEM((2, ny, nz), F32),
            pltpu.VMEM((2, ny, nz), F32),
            pltpu.VMEM((2, 2, ny + 8, nz), F32),
            pltpu.VMEM((2, 2, ny + 8, nz), F32),
            pltpu.VMEM((2, 2, ny, nz), F32),
            pltpu.VMEM((2, 2, ny, nz), F32),
            pltpu.VMEM((2, 1, nz), F32),
            pltpu.VMEM((2, 1, nz), F32),
            pltpu.VMEM((2, 2, 1, nz), F32),
            pltpu.VMEM((2, 2, 1, nz), F32),
            pltpu.VMEM((2, 2, nx, nz), F32),
            pltpu.VMEM((2, 2, nx, nz), F32),
            pltpu.VMEM((2, ny, nz), F32),
            pltpu.VMEM((1, 1, nz), F32),
            pltpu.VMEM((devices, 1, nz), F32),
            pltpu.SMEM(wavelet.shape, F32),
            pltpu.SMEM((1,), jnp.int32),
            pltpu.SMEM((1,), jnp.int32),
            pltpu.VMEM((1, count), jnp.int32),
            pltpu.VMEM(residuals.shape, F32),
            pltpu.VMEM((1, 1, nz), F32),
            dma((11,)),
            dma((2, 12)),
            dma((2, 2, 12)),
            dma((2, 3)),
            dma((2, 3)),
            dma((devices,)),
            dma((devices,)),
            dma((devices,)),
            dma((devices,)),
        ],
        compiler_params=pltpu.CompilerParams(
            collective_id=0, has_side_effects=True, vmem_limit_bytes=60 * 1024 * 1024
        ),
    )(
        wavelet, source_cell, start_step, receiver_cells.reshape(1, count),
        permittivity, loss, fwd_electric, fwd_magnetic, adj_electric, adj_magnetic, residuals,
    )
    return direction, rms.reshape(())


def solution(mesh):
    block = P("gx", "gy", "gz")
    state = P(None, "gx", "gy", "gz")
    return jax.shard_map(
        per_device,
        mesh=mesh,
        in_specs=(
            block, block, state, state, state, state,
            P(), P(("gx", "gy", "gz"), None), P(), P(), P(),
        ),
        out_specs=(block, P()),
        check_vma=False,
    )
```

```python
import functools

import jax
import jax.numpy as jnp
from jax import lax
from jax.experimental import pallas as pl
from jax.experimental.pallas import tpu as pltpu
from jax.sharding import PartitionSpec as P

STEPS = 4
MESH = pl.DeviceIdType.MESH
F32 = jnp.float32
HALF = 0.5


def kernel(
    sizes,
    wav_hbm,
    src_hbm,
    start_hbm,
    cells_hbm,
    perm_hbm,
    loss_hbm,
    fe_hbm,
    fm_hbm,
    ae_hbm,
    am_hbm,
    res_hbm,
    out_ref,
    rms_ref,
    E,
    H,
    perm,
    loss,
    keep,
    curl,
    D,
    A,
    inj,
    spots,
    R_all,
    grad,
    HY,
    HP,
    xU,
    xD,
    ysU,
    ysD,
    yU,
    yD,
    yzU,
    yzD,
    zsU,
    zsD,
    zU,
    zD,
    zX,
    zXU,
    e1s,
    e2s,
    e1r,
    e2r,
    hys,
    hzs,
    part,
    sums,
    wav_ref,
    src_ref,
    start_ref,
    cells_ref,
    res_ref,
    mine,
    load_sem,
    f_send,
    f_recv,
    h_send,
    h_recv,
    g_send,
    g_recv,
    l_send,
    l_recv,
    r_send,
    r_recv,
):
    gx, gy, gz = sizes
    nx, ny, nz = perm.shape
    pad = H.shape[3] - ny
    own = slice(0, ny)
    above = slice(1, ny + 1)
    O = slice(pad, pad + ny)
    ix, iy, iz = lax.axis_index("gx"), lax.axis_index("gy"), lax.axis_index("gz")
    nplane = gx * gz
    spot = ix * gz + iz

    loads = [
        pltpu.make_async_copy(fe_hbm, E.at[0, :, :, own, :], load_sem.at[0]),
        pltpu.make_async_copy(ae_hbm, E.at[1, :, :, own, :], load_sem.at[1]),
        pltpu.make_async_copy(fm_hbm, H.at[0, :, 1 : nx + 1, O, :], load_sem.at[2]),
        pltpu.make_async_copy(am_hbm, H.at[1, :, 1 : nx + 1, O, :], load_sem.at[3]),
        pltpu.make_async_copy(loss_hbm, loss, load_sem.at[4]),
        pltpu.make_async_copy(perm_hbm, perm, load_sem.at[5]),
    ]
    small = [
        pltpu.make_async_copy(start_hbm, start_ref, load_sem.at[6]),
        pltpu.make_async_copy(res_hbm, res_ref, load_sem.at[7]),
        pltpu.make_async_copy(src_hbm, src_ref, load_sem.at[8]),
        pltpu.make_async_copy(wav_hbm, wav_ref, load_sem.at[9]),
        pltpu.make_async_copy(cells_hbm, cells_ref, load_sem.at[10]),
    ]
    for load in small:
        load.start()
    for load in loads:
        load.start()

    zero_plane = jnp.zeros((ny, nz), F32)
    zero_row = jnp.zeros((1, nz), F32)
    for s in range(2):
        for c in range(3):
            for p in range(nx):
                E[s, c, p, ny : ny + 1, :] = zero_row
        for c in (1, 2):
            H[s, c, 0, O, :] = zero_plane
    for buffer in (HY, HP, xU, xD, yU, yD, yzU, yzD, zU, zD, zX, zXU, e1r, e2r):
        buffer[...] = jnp.zeros(buffer.shape, F32)

    has = {
        "+x": ix < gx - 1, "-x": ix > 0, "+y": iy < gy - 1,
        "-y": iy > 0, "+z": iz < gz - 1, "-z": iz > 0,
    }
    flip = {"+": "-", "-": "+"}

    def route(steps):
        dev = [ix, iy, iz]
        size = (gx, gy, gz)
        can_send, can_recv = True, True
        for step in steps:
            axis = "xyz".index(step[1])
            dev[axis] = jnp.clip(dev[axis] + (1 if step[0] == "+" else -1), 0, size[axis] - 1)
            back = flip[step[0]] + step[1]
            can_send = has[step] if can_send is True else can_send & has[step]
            can_recv = has[back] if can_recv is True else can_recv & has[back]
        return tuple(dev), can_send, can_recv

    layer = []
    for d in range(1, nplane):
        q = lax.rem(spot + d, nplane)
        layer.append((q, (q // gz, iy, lax.rem(q, gz))))
    line = []
    for d in range(1, gy):
        q = lax.rem(iy + d, gy)
        line.append((q, (ix, q, iz)))
    barrier = pltpu.get_barrier_semaphore()
    greeted = len(layer) + len(line)
    for steps in (("+x", "-y"), ("-x", "+y"), ("+y", "-z"), ("-y", "+z")):
        dev, can_send, _ = route(steps)
        greeted = greeted + can_send.astype(jnp.int32)

        @pl.when(can_send)
        def _():
            pl.semaphore_signal(barrier, inc=1, device_id=dev, device_id_type=MESH)

    for _, dev in layer + line:
        pl.semaphore_signal(barrier, inc=1, device_id=dev, device_id_type=MESH)

    lane = lax.broadcasted_iota(jnp.int32, (ny, nz), 1)
    row = lax.broadcasted_iota(jnp.int32, (ny, nz), 0)
    lane_p = lax.broadcasted_iota(jnp.int32, (nx, nz), 1)
    row_p = lax.broadcasted_iota(jnp.int32, (nx, nz), 0)

    per, trace = res_hbm.shape
    small[0].wait()
    small[1].wait()
    begin = start_ref[0]
    time_at = lax.broadcasted_iota(jnp.int32, (trace, nz), 0)
    turn = lax.div(lax.broadcasted_iota(jnp.int32, (trace, nz), 1), per)
    pick = jnp.where(time_at == begin + STEPS - 1 - turn, 1.0, 0.0)
    found = jnp.dot(res_ref[...], pick, precision=lax.Precision.HIGHEST, preferred_element_type=F32)
    mask = lax.rem(lax.broadcasted_iota(jnp.int32, (per, nz), 1), per)
    mask = mask == lax.broadcasted_iota(jnp.int32, (per, nz), 0)
    mine[0] = jnp.sum(jnp.where(mask, found, 0.0), axis=0, keepdims=True)
    R_all[pl.ds(iy * nplane + spot, 1)] = mine[...]
    for load in small[2:]:
        load.wait()
    pl.semaphore_wait(barrier, greeted)

    def remote(src, dst, ssem, rsem, dev):
        return pltpu.make_async_remote_copy(
            src_ref=src, dst_ref=dst, send_sem=ssem, recv_sem=rsem,
            device_id=dev, device_id_type=MESH,
        )

    def exchange(peers, at, src, slots, send_sems, recv_sems):
        copies = []
        for d, (q, dev) in enumerate(peers):
            send = remote(src, slots(at), send_sems.at[d], recv_sems.at[at], dev)
            recv = remote(src, slots(q), send_sems.at[d], recv_sems.at[q], dev)
            send.start()
            copies.append((send, recv))
        return copies

    def settle(copies):
        for send, recv in copies:
            recv.wait_recv()
        for send, recv in copies:
            send.wait_send()

    def face(s, slot, d):
        table = (
            (("+x",), E.at[s, :, nx - 1, own, :], xU.at[slot, s, :, own, :]),
            (("-x",), E.at[s, 1:3, 0, own, :], xD.at[slot, s]),
            (("+y",), ysU.at[s], yU.at[slot, s, :, 0:nx, :]),
            (("-y",), ysD.at[s], yD.at[slot, s]),
            (("+z",), zsU.at[s], zU.at[slot, s, own, :]),
            (("-z",), zsD.at[s], zD.at[slot, s]),
            (("+x", "-y"), e1s.at[s], e1r.at[slot, s]),
            (("-x", "+y"), e2s.at[s], e2r.at[slot, s]),
            (("+x", "-z"), E.at[s, 0, nx - 1, own, :], zX.at[slot, s]),
            (("-x", "+z"), E.at[s, 2, 0, own, :], zXU.at[slot, s]),
            (("+y", "-z"), ysU.at[s, 1], yzU.at[slot, s]),
            (("-y", "+z"), ysD.at[s, 1], yzD.at[slot, s]),
        )
        steps, source, target = table[d]
        dev, can_send, can_recv = route(steps)
        return remote(source, target, f_send.at[s, d], f_recv.at[slot, s, d], dev), can_send, can_recv

    def first(s, d):
        table = (
            (("+x",), H.at[s, 1:3, nx, O, :], H.at[s, 1:3, 0, O, :]),
            (("+y",), hys.at[s], HY.at[s]),
            (("+z",), hzs.at[s], HP.at[s]),
        )
        steps, source, target = table[d]
        dev, can_send, can_recv = route(steps)
        return remote(source, target, h_send.at[s, d], h_recv.at[s, d], dev), can_send, can_recv

    def start(item, extra=None):
        copy, can_send, _ = item

        @pl.when(can_send if extra is None else can_send & extra)
        def _():
            copy.start()

    def finish(item):
        copy, can_send, _ = item

        @pl.when(can_send)
        def _():
            copy.wait_send()

    def arrive(item):
        copy, _, can_recv = item

        @pl.when(can_recv)
        def _():
            copy.wait_recv()

    def pack_column(acc, value, source, j):
        return jnp.where(lane == j, pltpu.roll(value, (j - source) % nz, 1), acc)

    def up_z(value, halo, j):
        return jnp.where(lane == nz - 1, pltpu.roll(halo, (nz - 1 - j) % nz, 1), pltpu.roll(value, nz - 1, 1))

    def down_z(value, halo, j):
        rolled = pltpu.roll(value, 1, 1)
        return jnp.where(lane == 0, pltpu.roll(halo, (nz - j) % nz, 1), rolled)

    def pack_rows(s, p, ex, ey, ez):
        ysU[s, 0, p : p + 1, :] = ex[ny - 1 : ny, :]
        ysU[s, 1, p : p + 1, :] = ey[ny - 1 : ny, :]
        ysU[s, 2, p : p + 1, :] = ez[ny - 1 : ny, :]
        ysD[s, 0, p : p + 1, :] = ex[0:1, :]
        ysD[s, 1, p : p + 1, :] = ez[0:1, :]
        if p == nx - 1:
            e1s[s] = ex[0:1, :]
        if p == 0:
            e2s[s] = ey[ny - 1 : ny, :]

    def pack_low(s):
        acc = jnp.zeros((ny, nz), F32)
        for p in range(nx):
            acc = pack_column(acc, E[s, 0, p, own, :], 0, p)
            acc = pack_column(acc, E[s, 1, p, own, :], 0, nx + p)
        zsD[s] = acc

    def pack_high(s):
        acc = jnp.zeros((ny, nz), F32)
        for p in range(nx):
            acc = pack_column(acc, E[s, 0, p, own, :], nz - 1, p)
            acc = pack_column(acc, E[s, 1, p, own, :], nz - 1, nx + p)
            acc = pack_column(acc, E[s, 2, p, own, :], nz - 1, 2 * nx + p)
        zsU[s] = acc

    def send_z(s, slot, extra=None):
        for sign, pack, d in (("-z", pack_low, 5), ("+z", pack_high, 4)):
            @pl.when(has[sign] if extra is None else has[sign] & extra)
            def _():
                pack(s)
                face(s, slot, d)[0].start()

    def send_first(s):
        for d in (8, 9, 0, 1):
            start(face(s, 0, d))
        for p in range(nx):
            pack_rows(s, p, E[s, 0, p, own, :], E[s, 1, p, own, :], E[s, 2, p, own, :])
        for d in (10, 11, 6, 7, 2, 3):
            start(face(s, 0, d))
        send_z(s, 0)

    def send_magnetic(s):
        start(first(s, 0))
        for p in range(nx):
            hys[s, 0, p : p + 1, :] = H[s, 0, p + 1, pad + ny - 1 : pad + ny, :]
            hys[s, 1, p : p + 1, :] = H[s, 2, p + 1, pad + ny - 1 : pad + ny, :]
        start(first(s, 1))

        @pl.when(has["+z"])
        def _():
            acc = jnp.zeros((ny, nz), F32)
            for p in range(nx):
                acc = pack_column(acc, H[s, 1, p + 1, O, :], nz - 1, p)
                acc = pack_column(acc, H[s, 0, p + 1, O, :], nz - 1, nx + p)
            hzs[s] = acc
            first(s, 2)[0].start()

    half_x = jnp.where(has["-x"], HALF, 0.0)
    half_y = jnp.where(has["-y"], HALF, 0.0)

    def update_h(s, slot, opening):
        for d in (3, 5):
            arrive(face(s, slot, d))
        for p in range(nx):
            E[s, 0, p, ny : ny + 1, :] = yD[slot, s, 0, p : p + 1, :]
            E[s, 2, p, ny : ny + 1, :] = yD[slot, s, 1, p : p + 1, :]
        halo = zD[slot, s]
        for p in range(nx):
            if p == nx - 1:
                for d in (0, 1):
                    arrive(face(s, slot, d))
                next_y, next_z = xD[slot, s, 0], xD[slot, s, 1]
            else:
                next_y, next_z = E[s, 1, p + 1, own, :], E[s, 2, p + 1, own, :]
            ex, ey, ez = E[s, 0, p, own, :], E[s, 1, p, own, :], E[s, 2, p, own, :]
            hx = H[s, 0, p + 1, O, :] - HALF * (E[s, 2, p, above, :] - ez - (up_z(ey, halo, nx + p) - ey))
            hy = H[s, 1, p + 1, O, :] - HALF * (up_z(ex, halo, p) - ex - (next_z - ez))
            hz = H[s, 2, p + 1, O, :] - HALF * (next_y - ey - (E[s, 0, p, above, :] - ex))
            H[s, 0, p + 1, O, :] = hx
            H[s, 1, p + 1, O, :] = hy
            H[s, 2, p + 1, O, :] = hz
        for d in (2, 6, 7, 8, 10):
            arrive(face(s, slot, d))
        if opening:
            arrive(first(s, 0))
            arrive(first(s, 1))
        xU[slot, s, 0, ny : ny + 1, :] = e1r[slot, s]
        yU[slot, s, 1, nx : nx + 1, :] = e2r[slot, s]
        ex, ey, ez = xU[slot, s, 0, own, :], xU[slot, s, 1, own, :], xU[slot, s, 2, own, :]
        side_y = H[s, 1, 0, O, :] - half_x * (up_z(ex, zX[slot, s], 0) - ex - (E[s, 2, 0, own, :] - ez))
        side_z = H[s, 2, 0, O, :] - half_x * (E[s, 1, 0, own, :] - ey - (xU[slot, s, 0, above, :] - ex))
        H[s, 1, 0, O, :] = side_y
        H[s, 2, 0, O, :] = side_z
        ex, ey, ez = yU[slot, s, 0, 0:nx, :], yU[slot, s, 1, 0:nx, :], yU[slot, s, 2, 0:nx, :]
        far = jnp.where(lane_p == nz - 1, pltpu.roll(yzU[slot, s], nz - 1, 1), pltpu.roll(ey, nz - 1, 1))
        hx = HY[s, 0] - half_y * (ysD[s, 1] - ez - (far - ey))
        hz = HY[s, 1] - half_y * (yU[slot, s, 1, 1 : nx + 1, :] - ey - (ysD[s, 0] - ex))
        HY[s, 0] = hx
        HY[s, 1] = hz
        for p in range(nx):
            H[s, 0, p + 1, pad - 1 : pad, :] = hx[p : p + 1, :]
            H[s, 2, p + 1, pad - 1 : pad, :] = hz[p : p + 1, :]
        for d in (4, 9, 11):
            arrive(face(s, slot, d))
        if opening:
            arrive(first(s, 2))

        @pl.when(has["-z"])
        def _():
            edge = jnp.broadcast_to(yzD[slot, s, :, nz - 1 : nz], (nx, nz))
            edge = jnp.where(lane_p == 2 * nx + row_p, edge, 0.0)
            zU[slot, s, ny : ny + 1, :] = jnp.sum(edge, axis=0, keepdims=True)
            below = zU[slot, s, own, :]
            wide = jnp.where(lane == 3 * nx, pltpu.roll(zXU[slot, s], (3 * nx + 1) % nz, 1), below)
            along = pltpu.roll(pltpu.roll(wide, nz - 1, 1) - wide, nz - 2 * nx, 1)
            across = pltpu.roll(zU[slot, s, above, :] - below, nz - nx, 1)
            change = jnp.where(lane < nx, along, across)
            HP[s] = HP[s] - jnp.where(lane < nx, HALF, -HALF) * (zsD[s] - below - change)

    src = src_ref[0]
    total_z, total_y = nz * gz, ny * gy
    src_i = lax.div(src, total_y * total_z) - ix * nx
    src_j = lax.rem(lax.div(src, total_z), total_y) - iy * ny
    src_k = lax.rem(src, total_z) - iz * nz
    src_mask = (row == src_j) & (lane == src_k)

    def update_e(s, k, slot):
        for d in range(12):
            finish(face(s, slot, d))
        more = k < STEPS - 1
        halo = HP[s]
        below = slice(pad - 1, pad + ny - 1)
        pulse = wav_ref[begin + k]
        for p in (nx - 1,) + tuple(range(nx - 1)):
            hx, hy, hz = H[s, 0, p + 1, O, :], H[s, 1, p + 1, O, :], H[s, 2, p + 1, O, :]
            kp, cl = keep[p], curl[p]
            ox, oy, oz = E[s, 0, p, own, :], E[s, 1, p, own, :], E[s, 2, p, own, :]
            ex = kp * ox + cl * (hz - H[s, 2, p + 1, below, :] - (hy - down_z(hy, halo, p)))
            ey = kp * oy + cl * (hx - down_z(hx, halo, nx + p) - (hz - H[s, 2, p, O, :]))
            ez = kp * oz + cl * (hy - H[s, 1, p, O, :] - (hx - H[s, 0, p + 1, below, :]))
            if s == 0:
                ez = ez + jnp.where(src_mask, jnp.where(src_i == p, pulse, 0.0), 0.0)
                D[k, 0, p] = ex - ox
                D[k, 1, p] = ey - oy
                D[k, 2, p] = ez - oz
            else:
                ez = ez + inj[k, p * ny : (p + 1) * ny, :]
                A[k, 0, p] = ex
                A[k, 1, p] = ey
                A[k, 2, p] = ez
            E[s, 0, p, own, :] = ex
            E[s, 1, p, own, :] = ey
            E[s, 2, p, own, :] = ez
            pack_rows(s, p, ex, ey, ez)
            if p == nx - 1:
                for d in (6, 8, 0):
                    start(face(s, 1 - slot, d), more)
            if p == 0:
                for d in (7, 9, 1):
                    start(face(s, 1 - slot, d), more)
        for d in (10, 11, 2, 3):
            start(face(s, 1 - slot, d), more)
        send_z(s, 1 - slot, more)

    count = cells_ref.shape[1]

    def place_cells():
        cells = cells_ref[...]
        i = lax.div(cells, total_y * total_z) - ix * nx
        j = lax.rem(lax.div(cells, total_z), total_y) - iy * ny
        inside = (i >= 0) & (i < nx) & (j >= 0) & (j < ny)
        where = jnp.where(inside, i * ny + j, -1)
        rows = lax.broadcasted_iota(jnp.int32, (nx * ny, count), 0)
        spots[...] = jnp.where(rows == where, 1.0, 0.0).astype(jnp.bfloat16)

    def inject(m):
        k = lax.rem(cells_ref[...], total_z) - iz * nz
        depth = lax.broadcasted_iota(jnp.int32, (nz, count), 0) == k
        nt = (((1,), (1,)), ((), ()))
        spread_lane = lax.broadcasted_iota(jnp.int32, (nz, count), 0)
        spread_rec = lax.rem(lax.broadcasted_iota(jnp.int32, (nz, count), 1), per)
        device = lax.div(lax.broadcasted_iota(jnp.int32, (gy * nplane, count), 1), per)
        at_x, at_y, at_z = device // (gy * gz), lax.rem(device // gz, gy), lax.rem(device, gz)
        holder = at_y * nplane + at_x * gz + at_z == lax.broadcasted_iota(jnp.int32, (gy * nplane, count), 0)
        spread = jnp.where(spread_lane == m * per + spread_rec, 1.0, 0.0)
        found = jnp.dot(R_all[:, 0, :], spread, precision=lax.Precision.HIGHEST, preferred_element_type=F32)
        samples = jnp.sum(jnp.where(holder, found, 0.0), axis=0, keepdims=True)
        rest = jnp.where(depth, samples, 0.0)
        total = jnp.zeros((nx * ny, nz), F32)
        for _ in range(3):
            head = rest.astype(jnp.bfloat16)
            rest = rest - head.astype(F32)
            total = total + lax.dot_general(spots[...], head, nt, preferred_element_type=F32)
        inj[m] = total

    gather = exchange(layer, spot, mine.at[0], lambda q: R_all.at[iy * nplane + q], g_send, g_recv)
    for s in range(2):
        loads[s].wait()
        send_first(s)
    for s in range(2):
        loads[2 + s].wait()
        send_magnetic(s)
    loads[4].wait()
    loads[5].wait()
    for p in range(nx):
        lo = loss[p]
        keep[p] = (1.0 - lo) / (1.0 + lo)
        curl[p] = 0.5 / (perm[p] * (1.0 + lo))
    settle(gather)
    block = R_all.at[pl.ds(iy * nplane, nplane)]
    gather = exchange(line, iy, block, lambda q: R_all.at[pl.ds(q * nplane, nplane)], l_send, l_recv)
    place_cells()

    for s in range(2):
        for d in range(3):
            finish(first(s, d))
        update_h(s, 0, True)
    update_e(0, 0, 0)
    settle(gather)
    inject(0)
    update_e(1, 0, 0)
    inject(1)

    def body(k, carry):
        slot = lax.rem(k, 2)
        for s in range(2):
            update_h(s, slot, False)
            update_e(s, k, slot)

        @pl.when(k < STEPS - 1)
        def _():
            inject(k + 1)

        return carry

    lax.fori_loop(1, STEPS, body, 0)

    squares = jnp.zeros((ny, nz), F32)
    for p in range(nx):
        total = jnp.zeros((ny, nz), F32)
        for m in range(STEPS):
            n = STEPS - 1 - m
            total = total + (D[n, 0, p] * A[m, 0, p] + D[n, 1, p] * A[m, 1, p] + D[n, 2, p] * A[m, 2, p])
        g = -total / perm[p]
        grad[p] = g
        squares = squares + g * g
    part[0] = jnp.sum(squares, axis=0, keepdims=True)
    devices = gy * nplane
    me = iy * nplane + spot
    peers = []
    for d in range(1, devices):
        q = lax.rem(me + d, devices)
        peers.append((q, (lax.rem(q // gz, gx), q // nplane, lax.rem(q, gz))))
    sums[pl.ds(me, 1)] = part[...]
    settle(exchange(peers, me, part.at[0], lambda q: sums.at[q], r_send, r_recv))
    tile = sums[:, 0, :]
    total = jnp.sum(jnp.sum(tile, axis=0, keepdims=True), axis=1, keepdims=True)
    rms = jnp.sqrt(total / (nx * ny * nz * gx * gy * gz) + 1e-06)
    rms_ref[...] = rms
    inverse = 1.0 / rms
    for p in range(nx):
        out_ref[p] = grad[p] * inverse


def per_device(
    permittivity, loss, fwd_electric, fwd_magnetic, adj_electric, adj_magnetic,
    wavelet, residuals, source_cell, receiver_cells, start_step,
):
    sizes = tuple(lax.axis_size(a) for a in ("gx", "gy", "gz"))
    gx, gy, gz = sizes
    nx, ny, nz = permittivity.shape
    devices = gx * gy * gz
    count = receiver_cells.shape[0]
    vmem = pl.BlockSpec(memory_space=pltpu.VMEM)
    hbm = pl.BlockSpec(memory_space=pltpu.HBM)
    dma = pltpu.SemaphoreType.DMA
    block = (nx, ny, nz)

    def room(*shape):
        return pltpu.VMEM(shape, F32)

    direction, rms = pl.pallas_call(
        functools.partial(kernel, sizes),
        out_shape=(
            pltpu.VMEM(block, F32),
            jax.ShapeDtypeStruct((1, 1), F32),
        ),
        in_specs=[hbm] * 11,
        out_specs=(vmem, vmem),
        scratch_shapes=[
            room(2, 3, nx, ny + 8, nz),
            room(2, 3, nx + 1, ny + 8, nz),
            room(*block),
            room(*block),
            room(*block),
            room(*block),
            room(STEPS, 3, *block),
            room(STEPS, 3, *block),
            room(STEPS, nx * ny, nz),
            pltpu.VMEM((nx * ny, count), jnp.bfloat16),
            room(devices, 1, nz),
            room(*block),
            room(2, 2, nx, nz),
            room(2, ny, nz),
            room(2, 2, 3, ny + 8, nz),
            room(2, 2, 2, ny, nz),
            room(2, 3, nx, nz),
            room(2, 2, nx, nz),
            room(2, 2, 3, nx + 8, nz),
            room(2, 2, 2, nx, nz),
            room(2, 2, nx, nz),
            room(2, 2, nx, nz),
            room(2, ny, nz),
            room(2, ny, nz),
            room(2, 2, ny + 8, nz),
            room(2, 2, ny, nz),
            room(2, 2, ny, nz),
            room(2, 2, ny, nz),
            room(2, 1, nz),
            room(2, 1, nz),
            room(2, 2, 1, nz),
            room(2, 2, 1, nz),
            room(2, 2, nx, nz),
            room(2, ny, nz),
            room(1, 1, nz),
            room(devices, 1, nz),
            pltpu.SMEM(wavelet.shape, F32),
            pltpu.SMEM((1,), jnp.int32),
            pltpu.SMEM((1,), jnp.int32),
            pltpu.VMEM((1, count), jnp.int32),
            room(*residuals.shape),
            room(1, 1, nz),
            dma((11,)),
            dma((2, 12)),
            dma((2, 2, 12)),
            dma((2, 3)),
            dma((2, 3)),
            dma((gx * gz,)),
            dma((gx * gz,)),
            dma((gy,)),
            dma((gy,)),
            dma((devices,)),
            dma((devices,)),
        ],
        compiler_params=pltpu.CompilerParams(
            collective_id=0, has_side_effects=True, vmem_limit_bytes=60 * 1024 * 1024
        ),
    )(
        wavelet, source_cell, start_step, receiver_cells.reshape(1, count),
        permittivity, loss, fwd_electric, fwd_magnetic, adj_electric, adj_magnetic, residuals,
    )
    return direction, rms.reshape(())


def solution(mesh):
    block = P("gx", "gy", "gz")
    state = P(None, "gx", "gy", "gz")
    return jax.shard_map(
        per_device,
        mesh=mesh,
        in_specs=(
            block, block, state, state, state, state,
            P(), P(("gx", "gy", "gz"), None), P(), P(), P(),
        ),
        out_specs=(block, P()),
        check_vma=False,
    )
```

```python
import functools

import jax
import jax.numpy as jnp
from jax import lax
from jax.experimental import pallas as pl
from jax.experimental.pallas import tpu as pltpu
from jax.sharding import PartitionSpec as P

STEPS = 4
MESH = pl.DeviceIdType.MESH
F32 = jnp.float32
HALF = 0.5


def kernel(
    sizes,
    wav_hbm,
    src_hbm,
    start_hbm,
    cells_hbm,
    perm_hbm,
    loss_hbm,
    fe_hbm,
    fm_hbm,
    ae_hbm,
    am_hbm,
    res_hbm,
    out_ref,
    rms_ref,
    E,
    H,
    perm,
    loss,
    keep,
    curl,
    D,
    A,
    inj,
    late,
    late_z,
    spots,
    spots_z,
    R_all,
    grad,
    HY,
    HP,
    xU,
    xD,
    ysU,
    ysD,
    yU,
    yD,
    yzU,
    yzD,
    zsU,
    zsD,
    zU,
    zD,
    zX,
    zXU,
    e1s,
    e2s,
    e1r,
    e2r,
    hys,
    hzs,
    part,
    sums,
    wav_ref,
    src_ref,
    start_ref,
    cells_ref,
    res_ref,
    mine,
    load_sem,
    f_send,
    f_recv,
    h_send,
    h_recv,
    g_send,
    g_recv,
    l_send,
    l_recv,
    r_send,
    r_recv,
):
    gx, gy, gz = sizes
    nx, ny, nz = perm.shape
    pad = H.shape[3] - ny
    own = slice(0, ny)
    above = slice(1, ny + 1)
    O = slice(pad, pad + ny)
    ix, iy, iz = lax.axis_index("gx"), lax.axis_index("gy"), lax.axis_index("gz")
    nplane = gx * gz
    spot = ix * gz + iz

    loads = [
        pltpu.make_async_copy(fe_hbm, E.at[0, :, :, own, :], load_sem.at[0]),
        pltpu.make_async_copy(ae_hbm, E.at[1, :, :, own, :], load_sem.at[1]),
        pltpu.make_async_copy(fm_hbm, H.at[0, :, 1 : nx + 1, O, :], load_sem.at[2]),
        pltpu.make_async_copy(am_hbm, H.at[1, :, 1 : nx + 1, O, :], load_sem.at[3]),
        pltpu.make_async_copy(loss_hbm, loss, load_sem.at[4]),
        pltpu.make_async_copy(perm_hbm, perm, load_sem.at[5]),
    ]
    small = [
        pltpu.make_async_copy(start_hbm, start_ref, load_sem.at[6]),
        pltpu.make_async_copy(res_hbm, res_ref, load_sem.at[7]),
        pltpu.make_async_copy(src_hbm, src_ref, load_sem.at[8]),
        pltpu.make_async_copy(wav_hbm, wav_ref, load_sem.at[9]),
        pltpu.make_async_copy(cells_hbm, cells_ref, load_sem.at[10]),
    ]
    for load in small:
        load.start()
    for load in loads:
        load.start()

    zero_plane = jnp.zeros((ny, nz), F32)
    zero_row = jnp.zeros((1, nz), F32)
    for s in range(2):
        for c in range(3):
            for p in range(nx):
                E[s, c, p, ny : ny + 1, :] = zero_row
        for c in (1, 2):
            H[s, c, 0, O, :] = zero_plane
    for buffer in (HY, HP, xU, xD, yU, yD, yzU, yzD, zU, zD, zX, zXU, e1r, e2r):
        buffer[...] = jnp.zeros(buffer.shape, F32)

    has = {
        "+x": ix < gx - 1, "-x": ix > 0, "+y": iy < gy - 1,
        "-y": iy > 0, "+z": iz < gz - 1, "-z": iz > 0,
    }
    flip = {"+": "-", "-": "+"}

    def route(steps):
        dev = [ix, iy, iz]
        size = (gx, gy, gz)
        can_send, can_recv = True, True
        for step in steps:
            axis = "xyz".index(step[1])
            dev[axis] = jnp.clip(dev[axis] + (1 if step[0] == "+" else -1), 0, size[axis] - 1)
            back = flip[step[0]] + step[1]
            can_send = has[step] if can_send is True else can_send & has[step]
            can_recv = has[back] if can_recv is True else can_recv & has[back]
        return tuple(dev), can_send, can_recv

    layer = []
    for d in range(1, nplane):
        q = lax.rem(spot + d, nplane)
        layer.append((q, (q // gz, iy, lax.rem(q, gz))))
    line = []
    for d in range(1, gy):
        q = lax.rem(iy + d, gy)
        line.append((q, (ix, q, iz)))
    barrier = pltpu.get_barrier_semaphore()
    greeted = len(layer) + len(line)
    for steps in (("+x", "-y"), ("-x", "+y"), ("+y", "-z"), ("-y", "+z")):
        dev, can_send, _ = route(steps)
        greeted = greeted + can_send.astype(jnp.int32)

        @pl.when(can_send)
        def _():
            pl.semaphore_signal(barrier, inc=1, device_id=dev, device_id_type=MESH)

    for _, dev in layer + line:
        pl.semaphore_signal(barrier, inc=1, device_id=dev, device_id_type=MESH)

    lane = lax.broadcasted_iota(jnp.int32, (ny, nz), 1)
    row = lax.broadcasted_iota(jnp.int32, (ny, nz), 0)
    lane_p = lax.broadcasted_iota(jnp.int32, (nx, nz), 1)
    row_p = lax.broadcasted_iota(jnp.int32, (nx, nz), 0)

    per, trace = res_hbm.shape
    small[0].wait()
    small[1].wait()
    begin = start_ref[0]
    time_at = lax.broadcasted_iota(jnp.int32, (trace, nz), 0)
    turn = lax.div(lax.broadcasted_iota(jnp.int32, (trace, nz), 1), per)
    pick = jnp.where(time_at == begin + STEPS - 1 - turn, 1.0, 0.0)
    found = jnp.dot(res_ref[...], pick, precision=lax.Precision.HIGHEST, preferred_element_type=F32)
    mask = lax.rem(lax.broadcasted_iota(jnp.int32, (per, nz), 1), per)
    mask = mask == lax.broadcasted_iota(jnp.int32, (per, nz), 0)
    mine[0] = jnp.sum(jnp.where(mask, found, 0.0), axis=0, keepdims=True)
    R_all[pl.ds(iy * nplane + spot, 1)] = mine[...]
    for load in small[2:]:
        load.wait()
    pl.semaphore_wait(barrier, greeted)

    def remote(src, dst, ssem, rsem, dev):
        return pltpu.make_async_remote_copy(
            src_ref=src, dst_ref=dst, send_sem=ssem, recv_sem=rsem,
            device_id=dev, device_id_type=MESH,
        )

    def exchange(peers, at, src, slots, send_sems, recv_sems):
        copies = []
        for d, (q, dev) in enumerate(peers):
            send = remote(src, slots(at), send_sems.at[d], recv_sems.at[at], dev)
            recv = remote(src, slots(q), send_sems.at[d], recv_sems.at[q], dev)
            send.start()
            copies.append((send, recv))
        return copies

    def settle(copies):
        for send, recv in copies:
            recv.wait_recv()
        for send, recv in copies:
            send.wait_send()

    def face(s, slot, d):
        table = (
            (("+x",), E.at[s, :, nx - 1, own, :], xU.at[slot, s, :, own, :]),
            (("-x",), E.at[s, 1:3, 0, own, :], xD.at[slot, s]),
            (("+y",), ysU.at[s], yU.at[slot, s, :, 0:nx, :]),
            (("-y",), ysD.at[s], yD.at[slot, s]),
            (("+z",), zsU.at[s], zU.at[slot, s, own, :]),
            (("-z",), zsD.at[s], zD.at[slot, s]),
            (("+x", "-y"), e1s.at[s], e1r.at[slot, s]),
            (("-x", "+y"), e2s.at[s], e2r.at[slot, s]),
            (("+x", "-z"), E.at[s, 0, nx - 1, own, :], zX.at[slot, s]),
            (("-x", "+z"), E.at[s, 2, 0, own, :], zXU.at[slot, s]),
            (("+y", "-z"), ysU.at[s, 1], yzU.at[slot, s]),
            (("-y", "+z"), ysD.at[s, 1], yzD.at[slot, s]),
        )
        steps, source, target = table[d]
        dev, can_send, can_recv = route(steps)
        return remote(source, target, f_send.at[s, d], f_recv.at[slot, s, d], dev), can_send, can_recv

    def first(s, d):
        table = (
            (("+x",), H.at[s, 1:3, nx, O, :], H.at[s, 1:3, 0, O, :]),
            (("+y",), hys.at[s], HY.at[s]),
            (("+z",), hzs.at[s], HP.at[s]),
        )
        steps, source, target = table[d]
        dev, can_send, can_recv = route(steps)
        return remote(source, target, h_send.at[s, d], h_recv.at[s, d], dev), can_send, can_recv

    def start(item, extra=None):
        copy, can_send, _ = item

        @pl.when(can_send if extra is None else can_send & extra)
        def _():
            copy.start()

    def finish(item):
        copy, can_send, _ = item

        @pl.when(can_send)
        def _():
            copy.wait_send()

    def arrive(item):
        copy, _, can_recv = item

        @pl.when(can_recv)
        def _():
            copy.wait_recv()

    def pack_column(acc, value, source, j):
        return jnp.where(lane == j, pltpu.roll(value, (j - source) % nz, 1), acc)

    def up_z(value, halo, j):
        return jnp.where(lane == nz - 1, pltpu.roll(halo, (nz - 1 - j) % nz, 1), pltpu.roll(value, nz - 1, 1))

    def down_z(value, halo, j):
        rolled = pltpu.roll(value, 1, 1)
        return jnp.where(lane == 0, pltpu.roll(halo, (nz - j) % nz, 1), rolled)

    def pack_rows(s, p, ex, ey, ez):
        ysU[s, 0, p : p + 1, :] = ex[ny - 1 : ny, :]
        ysU[s, 1, p : p + 1, :] = ey[ny - 1 : ny, :]
        ysU[s, 2, p : p + 1, :] = ez[ny - 1 : ny, :]
        ysD[s, 0, p : p + 1, :] = ex[0:1, :]
        ysD[s, 1, p : p + 1, :] = ez[0:1, :]
        if p == nx - 1:
            e1s[s] = ex[0:1, :]
        if p == 0:
            e2s[s] = ey[ny - 1 : ny, :]

    def pack_low(s):
        acc = jnp.zeros((ny, nz), F32)
        for p in range(nx):
            acc = pack_column(acc, E[s, 0, p, own, :], 0, p)
            acc = pack_column(acc, E[s, 1, p, own, :], 0, nx + p)
        zsD[s] = acc

    def pack_high(s):
        acc = jnp.zeros((ny, nz), F32)
        for p in range(nx):
            acc = pack_column(acc, E[s, 0, p, own, :], nz - 1, p)
            acc = pack_column(acc, E[s, 1, p, own, :], nz - 1, nx + p)
            acc = pack_column(acc, E[s, 2, p, own, :], nz - 1, 2 * nx + p)
        zsU[s] = acc

    def send_z(s, slot, extra=None):
        for sign, pack, d in (("-z", pack_low, 5), ("+z", pack_high, 4)):
            @pl.when(has[sign] if extra is None else has[sign] & extra)
            def _():
                pack(s)
                face(s, slot, d)[0].start()

    def send_first(s):
        for d in (8, 9, 0, 1):
            start(face(s, 0, d))
        for p in range(nx):
            pack_rows(s, p, E[s, 0, p, own, :], E[s, 1, p, own, :], E[s, 2, p, own, :])
        for d in (10, 11, 6, 7, 2, 3):
            start(face(s, 0, d))
        send_z(s, 0)

    def send_magnetic(s):
        start(first(s, 0))
        for p in range(nx):
            hys[s, 0, p : p + 1, :] = H[s, 0, p + 1, pad + ny - 1 : pad + ny, :]
            hys[s, 1, p : p + 1, :] = H[s, 2, p + 1, pad + ny - 1 : pad + ny, :]
        start(first(s, 1))

        @pl.when(has["+z"])
        def _():
            acc = jnp.zeros((ny, nz), F32)
            for p in range(nx):
                acc = pack_column(acc, H[s, 1, p + 1, O, :], nz - 1, p)
                acc = pack_column(acc, H[s, 0, p + 1, O, :], nz - 1, nx + p)
            hzs[s] = acc
            first(s, 2)[0].start()

    half_x = jnp.where(has["-x"], HALF, 0.0)
    half_y = jnp.where(has["-y"], HALF, 0.0)

    base = nx * ny
    rim = base + 2 * ny + 2 * nx

    def add_late(slot):
        for d in range(12):
            finish(face(1, slot, d))
        for p in range(nx):
            extra = late[p * ny : (p + 1) * ny, :]
            E[1, 2, p, own, :] = E[1, 2, p, own, :] + extra
            A[0, 2, p] = A[0, 2, p] + extra

    def update_h(s, slot, opening, behind=False):
        if behind:
            add_late(slot)
        for d in (3, 5):
            arrive(face(s, slot, d))
        for p in range(nx):
            E[s, 0, p, ny : ny + 1, :] = yD[slot, s, 0, p : p + 1, :]
            if behind:
                at = base + 2 * ny + nx + p
                E[s, 2, p, ny : ny + 1, :] = yD[slot, s, 1, p : p + 1, :] + late[at : at + 1, :]
            else:
                E[s, 2, p, ny : ny + 1, :] = yD[slot, s, 1, p : p + 1, :]
        halo = zD[slot, s]
        for p in range(nx):
            if p == nx - 1:
                for d in (0, 1):
                    arrive(face(s, slot, d))
                next_y, next_z = xD[slot, s, 0], xD[slot, s, 1]
                if behind:
                    next_z = next_z + late[base + ny : base + 2 * ny, :]
            else:
                next_y, next_z = E[s, 1, p + 1, own, :], E[s, 2, p + 1, own, :]
            ex, ey, ez = E[s, 0, p, own, :], E[s, 1, p, own, :], E[s, 2, p, own, :]
            hx = H[s, 0, p + 1, O, :] - HALF * (E[s, 2, p, above, :] - ez - (up_z(ey, halo, nx + p) - ey))
            hy = H[s, 1, p + 1, O, :] - HALF * (up_z(ex, halo, p) - ex - (next_z - ez))
            hz = H[s, 2, p + 1, O, :] - HALF * (next_y - ey - (E[s, 0, p, above, :] - ex))
            H[s, 0, p + 1, O, :] = hx
            H[s, 1, p + 1, O, :] = hy
            H[s, 2, p + 1, O, :] = hz
        for d in (2, 6, 7, 8, 10):
            arrive(face(s, slot, d))
        if opening:
            arrive(first(s, 0))
            arrive(first(s, 1))
        xU[slot, s, 0, ny : ny + 1, :] = e1r[slot, s]
        yU[slot, s, 1, nx : nx + 1, :] = e2r[slot, s]
        ex, ey, ez = xU[slot, s, 0, own, :], xU[slot, s, 1, own, :], xU[slot, s, 2, own, :]
        if behind:
            ez = ez + late[base : base + ny, :]
        side_y = H[s, 1, 0, O, :] - half_x * (up_z(ex, zX[slot, s], 0) - ex - (E[s, 2, 0, own, :] - ez))
        side_z = H[s, 2, 0, O, :] - half_x * (E[s, 1, 0, own, :] - ey - (xU[slot, s, 0, above, :] - ex))
        H[s, 1, 0, O, :] = side_y
        H[s, 2, 0, O, :] = side_z
        ex, ey, ez = yU[slot, s, 0, 0:nx, :], yU[slot, s, 1, 0:nx, :], yU[slot, s, 2, 0:nx, :]
        far = jnp.where(lane_p == nz - 1, pltpu.roll(yzU[slot, s], nz - 1, 1), pltpu.roll(ey, nz - 1, 1))
        near = ysD[s, 1]
        if behind:
            ez = ez + late[base + 2 * ny : base + 2 * ny + nx, :]
            near = near + late[rim : rim + nx, :]
        hx = HY[s, 0] - half_y * (near - ez - (far - ey))
        hz = HY[s, 1] - half_y * (yU[slot, s, 1, 1 : nx + 1, :] - ey - (ysD[s, 0] - ex))
        HY[s, 0] = hx
        HY[s, 1] = hz
        for p in range(nx):
            H[s, 0, p + 1, pad - 1 : pad, :] = hx[p : p + 1, :]
            H[s, 2, p + 1, pad - 1 : pad, :] = hz[p : p + 1, :]
        for d in (4, 9, 11):
            arrive(face(s, slot, d))
        if opening:
            arrive(first(s, 2))

        @pl.when(has["-z"])
        def _():
            edge, far_x = yzD[slot, s], zXU[slot, s]
            if behind:
                edge = edge + late_z[ny : ny + nx, :]
                far_x = far_x + late_z[0:ny, :]
                zU[slot, s, own, :] = zU[slot, s, own, :] + late_z[0:ny, :]
            edge = jnp.broadcast_to(edge[:, nz - 1 : nz], (nx, nz))
            edge = jnp.sum(jnp.where(lane_p == nx + row_p, edge, 0.0), axis=0, keepdims=True)
            below = zU[slot, s, own, :]
            next_i = jnp.where(lane == nx - 1, pltpu.roll(far_x, nx, 1), pltpu.roll(below, nz - 2 * nx - 1, 1))
            next_j = jnp.where(row == ny - 1, edge, pltpu.roll(zU[slot, s, above, :], nz - nx, 1))
            along = next_i - pltpu.roll(below, nz - 2 * nx, 1)
            across = next_j - pltpu.roll(below, nz - nx, 1)
            change = jnp.where(lane < nx, along, across)
            HP[s] = HP[s] - jnp.where(lane < nx, HALF, -HALF) * (zsD[s] - below - change)

    src = src_ref[0]
    total_z, total_y = nz * gz, ny * gy
    src_i = lax.div(src, total_y * total_z) - ix * nx
    src_j = lax.rem(lax.div(src, total_z), total_y) - iy * ny
    src_k = lax.rem(src, total_z) - iz * nz
    src_mask = (row == src_j) & (lane == src_k)

    def update_e(s, k, slot, behind=False):
        if not behind:
            for d in range(12):
                finish(face(s, slot, d))
        more = k < STEPS - 1
        halo = HP[s]
        below = slice(pad - 1, pad + ny - 1)
        pulse = wav_ref[begin + k]
        for p in (nx - 1,) + tuple(range(nx - 1)):
            hx, hy, hz = H[s, 0, p + 1, O, :], H[s, 1, p + 1, O, :], H[s, 2, p + 1, O, :]
            kp, cl = keep[p], curl[p]
            ox, oy, oz = E[s, 0, p, own, :], E[s, 1, p, own, :], E[s, 2, p, own, :]
            ex = kp * ox + cl * (hz - H[s, 2, p + 1, below, :] - (hy - down_z(hy, halo, p)))
            ey = kp * oy + cl * (hx - down_z(hx, halo, nx + p) - (hz - H[s, 2, p, O, :]))
            ez = kp * oz + cl * (hy - H[s, 1, p, O, :] - (hx - H[s, 0, p + 1, below, :]))
            if s == 0:
                ez = ez + jnp.where(src_mask, jnp.where(src_i == p, pulse, 0.0), 0.0)
                D[k, 0, p] = ex - ox
                D[k, 1, p] = ey - oy
                D[k, 2, p] = ez - oz
            else:
                if not (isinstance(k, int) and k == 0):
                    ez = ez + inj[k, p * ny : (p + 1) * ny, :]
                A[k, 0, p] = ex
                A[k, 1, p] = ey
                A[k, 2, p] = ez
            E[s, 0, p, own, :] = ex
            E[s, 1, p, own, :] = ey
            E[s, 2, p, own, :] = ez
            pack_rows(s, p, ex, ey, ez)
            if p == nx - 1:
                for d in (6, 8, 0):
                    start(face(s, 1 - slot, d), more)
            if p == 0:
                for d in (7, 9, 1):
                    start(face(s, 1 - slot, d), more)
        for d in (10, 11, 2, 3):
            start(face(s, 1 - slot, d), more)
        send_z(s, 1 - slot, more)

    count = cells_ref.shape[1]

    def place_cells():
        cells = cells_ref[...]
        i = lax.div(cells, total_y * total_z) - ix * nx
        j = lax.rem(lax.div(cells, total_z), total_y) - iy * ny
        k = lax.rem(cells, total_z) - iz * nz
        in_x, in_y = (i >= 0) & (i < nx), (j >= 0) & (j < ny)
        where = jnp.where(in_x & in_y, i * ny + j, -1)
        where = jnp.where((i == -1) & in_y, base + j, where)
        where = jnp.where((i == nx) & in_y, base + ny + j, where)
        where = jnp.where((j == -1) & in_x, base + 2 * ny + i, where)
        where = jnp.where((j == ny) & in_x, base + 2 * ny + nx + i, where)
        again = jnp.where((j == 0) & in_x, rim + i, -1)
        rows = lax.broadcasted_iota(jnp.int32, spots.shape, 0)
        spots[...] = jnp.where((rows == where) | (rows == again), 1.0, 0.0).astype(jnp.bfloat16)
        where = jnp.where(in_y & (i >= 0) & (i <= nx) & (k == -1), j, -1)
        where = jnp.where((j == ny) & in_x & (k == -1), ny + i, where)
        rows = lax.broadcasted_iota(jnp.int32, spots_z.shape, 0)
        spots_z[...] = jnp.where(rows == where, 1.0, 0.0).astype(jnp.bfloat16)

    nt = (((1,), (1,)), ((), ()))

    def sampled(m):
        spread_lane = lax.broadcasted_iota(jnp.int32, (nz, count), 0)
        spread_rec = lax.rem(lax.broadcasted_iota(jnp.int32, (nz, count), 1), per)
        device = lax.div(lax.broadcasted_iota(jnp.int32, (gy * nplane, count), 1), per)
        at_x, at_y, at_z = device // (gy * gz), lax.rem(device // gz, gy), lax.rem(device, gz)
        holder = at_y * nplane + at_x * gz + at_z == lax.broadcasted_iota(jnp.int32, (gy * nplane, count), 0)
        spread = jnp.where(spread_lane == m * per + spread_rec, 1.0, 0.0)
        found = jnp.dot(R_all[:, 0, :], spread, precision=lax.Precision.HIGHEST, preferred_element_type=F32)
        return jnp.sum(jnp.where(holder, found, 0.0), axis=0, keepdims=True)

    def spread_out(rows, rest):
        total = jnp.zeros((rows.shape[0], nz), F32)
        for _ in range(3):
            head = rest.astype(jnp.bfloat16)
            rest = rest - head.astype(F32)
            total = total + lax.dot_general(rows, head, nt, preferred_element_type=F32)
        return total

    lane_c = lax.broadcasted_iota(jnp.int32, (nz, count), 0)

    def inject(m):
        k = lax.rem(cells_ref[...], total_z) - iz * nz
        inj[m] = spread_out(spots[0:base, :], jnp.where(lane_c == k, sampled(m), 0.0))

    def inject_late():
        cells = cells_ref[...]
        k = lax.rem(cells, total_z) - iz * nz
        i = lax.div(cells, total_y * total_z) - ix * nx
        samples = sampled(0)
        late[...] = spread_out(spots[...], jnp.where(lane_c == k, samples, 0.0))
        j = lax.rem(lax.div(cells, total_z), total_y) - iy * ny
        at = jnp.where((i == nx) | (j == ny), nz - 1, 2 * nx + i)
        late_z[...] = spread_out(spots_z[...], jnp.where(lane_c == at, samples, 0.0))

    gather = exchange(layer, spot, mine.at[0], lambda q: R_all.at[iy * nplane + q], g_send, g_recv)
    for s in range(2):
        loads[s].wait()
        send_first(s)
    for s in range(2):
        loads[2 + s].wait()
        send_magnetic(s)
    loads[4].wait()
    loads[5].wait()
    for p in range(nx):
        lo = loss[p]
        keep[p] = (1.0 - lo) / (1.0 + lo)
        curl[p] = 0.5 / (perm[p] * (1.0 + lo))
    settle(gather)
    block = R_all.at[pl.ds(iy * nplane, nplane)]
    gather = exchange(line, iy, block, lambda q: R_all.at[pl.ds(q * nplane, nplane)], l_send, l_recv)
    place_cells()

    for s in range(2):
        for d in range(3):
            finish(first(s, d))
        update_h(s, 0, True)
    update_e(0, 0, 0)
    update_e(1, 0, 0)
    settle(gather)
    inject_late()
    inject(1)
    update_h(0, 1, False)
    update_e(0, 1, 1)
    update_h(1, 1, False, True)
    update_e(1, 1, 1, True)
    inject(2)

    def body(k, carry):
        slot = lax.rem(k, 2)
        for s in range(2):
            update_h(s, slot, False)
            update_e(s, k, slot)

        @pl.when(k < STEPS - 1)
        def _():
            inject(k + 1)

        return carry

    lax.fori_loop(2, STEPS, body, 0)

    squares = jnp.zeros((ny, nz), F32)
    for p in range(nx):
        total = jnp.zeros((ny, nz), F32)
        for m in range(STEPS):
            n = STEPS - 1 - m
            total = total + (D[n, 0, p] * A[m, 0, p] + D[n, 1, p] * A[m, 1, p] + D[n, 2, p] * A[m, 2, p])
        g = -total / perm[p]
        grad[p] = g
        squares = squares + g * g
    part[0] = jnp.sum(squares, axis=0, keepdims=True)
    devices = gy * nplane
    me = iy * nplane + spot
    peers = []
    for d in range(1, devices):
        q = lax.rem(me + d, devices)
        peers.append((q, (lax.rem(q // gz, gx), q // nplane, lax.rem(q, gz))))
    sums[pl.ds(me, 1)] = part[...]
    settle(exchange(peers, me, part.at[0], lambda q: sums.at[q], r_send, r_recv))
    tile = sums[:, 0, :]
    total = jnp.sum(jnp.sum(tile, axis=0, keepdims=True), axis=1, keepdims=True)
    rms = jnp.sqrt(total / (nx * ny * nz * gx * gy * gz) + 1e-06)
    rms_ref[...] = rms
    inverse = 1.0 / rms
    for p in range(nx):
        out_ref[p] = grad[p] * inverse


def per_device(
    permittivity, loss, fwd_electric, fwd_magnetic, adj_electric, adj_magnetic,
    wavelet, residuals, source_cell, receiver_cells, start_step,
):
    sizes = tuple(lax.axis_size(a) for a in ("gx", "gy", "gz"))
    gx, gy, gz = sizes
    nx, ny, nz = permittivity.shape
    devices = gx * gy * gz
    count = receiver_cells.shape[0]
    vmem = pl.BlockSpec(memory_space=pltpu.VMEM)
    hbm = pl.BlockSpec(memory_space=pltpu.HBM)
    dma = pltpu.SemaphoreType.DMA
    block = (nx, ny, nz)

    extended = -(-(nx * ny + 2 * ny + 3 * nx) // 16) * 16
    flat = -(-(ny + nx) // 16) * 16

    def room(*shape):
        return pltpu.VMEM(shape, F32)

    direction, rms = pl.pallas_call(
        functools.partial(kernel, sizes),
        out_shape=(
            pltpu.VMEM(block, F32),
            jax.ShapeDtypeStruct((1, 1), F32),
        ),
        in_specs=[hbm] * 11,
        out_specs=(vmem, vmem),
        scratch_shapes=[
            room(2, 3, nx, ny + 8, nz),
            room(2, 3, nx + 1, ny + 8, nz),
            room(*block),
            room(*block),
            room(*block),
            room(*block),
            room(STEPS, 3, *block),
            room(STEPS, 3, *block),
            room(STEPS, nx * ny, nz),
            room(extended, nz),
            room(flat, nz),
            pltpu.VMEM((extended, count), jnp.bfloat16),
            pltpu.VMEM((flat, count), jnp.bfloat16),
            room(devices, 1, nz),
            room(*block),
            room(2, 2, nx, nz),
            room(2, ny, nz),
            room(2, 2, 3, ny + 8, nz),
            room(2, 2, 2, ny, nz),
            room(2, 3, nx, nz),
            room(2, 2, nx, nz),
            room(2, 2, 3, nx + 8, nz),
            room(2, 2, 2, nx, nz),
            room(2, 2, nx, nz),
            room(2, 2, nx, nz),
            room(2, ny, nz),
            room(2, ny, nz),
            room(2, 2, ny + 8, nz),
            room(2, 2, ny, nz),
            room(2, 2, ny, nz),
            room(2, 2, ny, nz),
            room(2, 1, nz),
            room(2, 1, nz),
            room(2, 2, 1, nz),
            room(2, 2, 1, nz),
            room(2, 2, nx, nz),
            room(2, ny, nz),
            room(1, 1, nz),
            room(devices, 1, nz),
            pltpu.SMEM(wavelet.shape, F32),
            pltpu.SMEM((1,), jnp.int32),
            pltpu.SMEM((1,), jnp.int32),
            pltpu.VMEM((1, count), jnp.int32),
            room(*residuals.shape),
            room(1, 1, nz),
            dma((11,)),
            dma((2, 12)),
            dma((2, 2, 12)),
            dma((2, 3)),
            dma((2, 3)),
            dma((gx * gz,)),
            dma((gx * gz,)),
            dma((gy,)),
            dma((gy,)),
            dma((devices,)),
            dma((devices,)),
        ],
        compiler_params=pltpu.CompilerParams(
            collective_id=0, has_side_effects=True, vmem_limit_bytes=60 * 1024 * 1024
        ),
    )(
        wavelet, source_cell, start_step, receiver_cells.reshape(1, count),
        permittivity, loss, fwd_electric, fwd_magnetic, adj_electric, adj_magnetic, residuals,
    )
    return direction, rms.reshape(())


def solution(mesh):
    block = P("gx", "gy", "gz")
    state = P(None, "gx", "gy", "gz")
    return jax.shard_map(
        per_device,
        mesh=mesh,
        in_specs=(
            block, block, state, state, state, state,
            P(), P(("gx", "gy", "gz"), None), P(), P(), P(),
        ),
        out_specs=(block, P()),
        check_vma=False,
    )
```

```python
import functools

import jax
import jax.numpy as jnp
from jax import lax
from jax.experimental import pallas as pl
from jax.experimental.pallas import tpu as pltpu
from jax.sharding import PartitionSpec as P

STEPS = 4
MESH = pl.DeviceIdType.MESH
F32 = jnp.float32
HALF = 0.5


def kernel(
    sizes,
    wav_hbm,
    src_hbm,
    start_hbm,
    cells_hbm,
    perm_hbm,
    loss_hbm,
    fe_hbm,
    fm_hbm,
    ae_hbm,
    am_hbm,
    res_hbm,
    out_ref,
    rms_ref,
    E,
    H,
    perm,
    loss,
    keep,
    curl,
    D,
    A,
    inj,
    late,
    late_z,
    spots,
    spots_z,
    R_all,
    grad,
    HY,
    HP,
    xU,
    xD,
    ysU,
    ysD,
    yU,
    yD,
    yzU,
    yzD,
    zsU,
    zsD,
    zU,
    zD,
    zX,
    zXU,
    e1s,
    e2s,
    e1r,
    e2r,
    hys,
    hzs,
    part,
    sums,
    wav_ref,
    src_ref,
    start_ref,
    cells_ref,
    res_ref,
    mine,
    load_sem,
    f_send,
    f_recv,
    h_send,
    h_recv,
    g_send,
    g_recv,
    l_send,
    l_recv,
    told,
    r_send,
    r_recv,
):
    gx, gy, gz = sizes
    nx, ny, nz = perm.shape
    pad = H.shape[3] - ny
    own = slice(0, ny)
    above = slice(1, ny + 1)
    O = slice(pad, pad + ny)
    ix, iy, iz = lax.axis_index("gx"), lax.axis_index("gy"), lax.axis_index("gz")
    nplane = gx * gz
    spot = ix * gz + iz

    loads = [
        pltpu.make_async_copy(fe_hbm, E.at[0, :, :, own, :], load_sem.at[0]),
        pltpu.make_async_copy(ae_hbm, E.at[1, :, :, own, :], load_sem.at[1]),
        pltpu.make_async_copy(fm_hbm, H.at[0, :, 1 : nx + 1, O, :], load_sem.at[2]),
        pltpu.make_async_copy(am_hbm, H.at[1, :, 1 : nx + 1, O, :], load_sem.at[3]),
        pltpu.make_async_copy(loss_hbm, loss, load_sem.at[4]),
        pltpu.make_async_copy(perm_hbm, perm, load_sem.at[5]),
    ]
    small = [
        pltpu.make_async_copy(start_hbm, start_ref, load_sem.at[6]),
        pltpu.make_async_copy(res_hbm, res_ref, load_sem.at[7]),
        pltpu.make_async_copy(src_hbm, src_ref, load_sem.at[8]),
        pltpu.make_async_copy(wav_hbm, wav_ref, load_sem.at[9]),
        pltpu.make_async_copy(cells_hbm, cells_ref, load_sem.at[10]),
    ]
    for load in small:
        load.start()
    for i in (0, 2, 1, 3, 4, 5):
        loads[i].start()

    zero_plane = jnp.zeros((ny, nz), F32)
    zero_row = jnp.zeros((1, nz), F32)
    for s in range(2):
        for c in range(3):
            for p in range(nx):
                E[s, c, p, ny : ny + 1, :] = zero_row
        for c in (1, 2):
            H[s, c, 0, O, :] = zero_plane
    for buffer in (HY, HP, xU, xD, yU, yD, yzU, yzD, zU, zD, zX, zXU, e1r, e2r):
        buffer[...] = jnp.zeros(buffer.shape, F32)

    has = {
        "+x": ix < gx - 1, "-x": ix > 0, "+y": iy < gy - 1,
        "-y": iy > 0, "+z": iz < gz - 1, "-z": iz > 0,
    }
    flip = {"+": "-", "-": "+"}

    def route(steps):
        dev = [ix, iy, iz]
        size = (gx, gy, gz)
        can_send, can_recv = True, True
        for step in steps:
            axis = "xyz".index(step[1])
            dev[axis] = jnp.clip(dev[axis] + (1 if step[0] == "+" else -1), 0, size[axis] - 1)
            back = flip[step[0]] + step[1]
            can_send = has[step] if can_send is True else can_send & has[step]
            can_recv = has[back] if can_recv is True else can_recv & has[back]
        return tuple(dev), can_send, can_recv

    layer = []
    for d in range(1, nplane):
        q = lax.rem(spot + d, nplane)
        layer.append((q, (q // gz, iy, lax.rem(q, gz))))
    line = []
    for d in range(1, gy):
        q = lax.rem(iy + d, gy)
        line.append((q, (ix, q, iz)))
    barrier = pltpu.get_barrier_semaphore()
    greeted = len(layer)
    beside = has["+y"].astype(jnp.int32) + has["-y"].astype(jnp.int32)
    for steps in (("+y",), ("-y",), ("+x", "-y"), ("-x", "+y"), ("+y", "-z"), ("-y", "+z")):
        dev, can_send, _ = route(steps)
        greeted = greeted + can_send.astype(jnp.int32)

        @pl.when(can_send)
        def _():
            pl.semaphore_signal(barrier, inc=1, device_id=dev, device_id_type=MESH)

    for _, dev in layer:
        pl.semaphore_signal(barrier, inc=1, device_id=dev, device_id_type=MESH)

    lane = lax.broadcasted_iota(jnp.int32, (ny, nz), 1)
    row = lax.broadcasted_iota(jnp.int32, (ny, nz), 0)
    lane_p = lax.broadcasted_iota(jnp.int32, (nx, nz), 1)
    row_p = lax.broadcasted_iota(jnp.int32, (nx, nz), 0)

    per, trace = res_hbm.shape
    small[0].wait()
    small[1].wait()
    begin = start_ref[0]
    time_at = lax.broadcasted_iota(jnp.int32, (trace, nz), 0)
    turn = lax.div(lax.broadcasted_iota(jnp.int32, (trace, nz), 1), per)
    pick = jnp.where(time_at == begin + STEPS - 1 - turn, 1.0, 0.0)
    found = jnp.dot(res_ref[...], pick, precision=lax.Precision.HIGHEST, preferred_element_type=F32)
    mask = lax.rem(lax.broadcasted_iota(jnp.int32, (per, nz), 1), per)
    mask = mask == lax.broadcasted_iota(jnp.int32, (per, nz), 0)
    mine[0] = jnp.sum(jnp.where(mask, found, 0.0), axis=0, keepdims=True)
    R_all[pl.ds(iy * nplane + spot, 1)] = mine[...]
    for load in small[2:]:
        load.wait()
    pl.semaphore_wait(barrier, greeted)

    def tell(step):
        for way in ("+y", "-y"):
            dev, can_send, _ = route((way,))

            @pl.when(can_send)
            def _():
                pl.semaphore_signal(told.at[step], inc=1, device_id=dev, device_id_type=MESH)

    hops = gy - 2
    if hops > 0:
        tell(0)

    def remote(src, dst, ssem, rsem, dev):
        return pltpu.make_async_remote_copy(
            src_ref=src, dst_ref=dst, send_sem=ssem, recv_sem=rsem,
            device_id=dev, device_id_type=MESH,
        )

    def exchange(peers, at, src, slots, send_sems, recv_sems):
        copies = []
        for d, (q, dev) in enumerate(peers):
            send = remote(src, slots(at), send_sems.at[d], recv_sems.at[at], dev)
            recv = remote(src, slots(q), send_sems.at[d], recv_sems.at[q], dev)
            send.start()
            copies.append((send, recv))
        return copies

    def settle(copies):
        for send, recv in copies:
            recv.wait_recv()
        for send, recv in copies:
            send.wait_send()

    def face(s, slot, d):
        table = (
            (("+x",), E.at[s, :, nx - 1, own, :], xU.at[slot, s, :, own, :]),
            (("-x",), E.at[s, 1:3, 0, own, :], xD.at[slot, s]),
            (("+y",), ysU.at[s], yU.at[slot, s, :, 0:nx, :]),
            (("-y",), ysD.at[s], yD.at[slot, s]),
            (("+z",), zsU.at[s], zU.at[slot, s, own, :]),
            (("-z",), zsD.at[s], zD.at[slot, s]),
            (("+x", "-y"), e1s.at[s], e1r.at[slot, s]),
            (("-x", "+y"), e2s.at[s], e2r.at[slot, s]),
            (("+x", "-z"), E.at[s, 0, nx - 1, own, :], zX.at[slot, s]),
            (("-x", "+z"), E.at[s, 2, 0, own, :], zXU.at[slot, s]),
            (("+y", "-z"), ysU.at[s, 1], yzU.at[slot, s]),
            (("-y", "+z"), ysD.at[s, 1], yzD.at[slot, s]),
        )
        steps, source, target = table[d]
        dev, can_send, can_recv = route(steps)
        return remote(source, target, f_send.at[s, d], f_recv.at[slot, s, d], dev), can_send, can_recv

    def first(s, d):
        table = (
            (("+x",), H.at[s, 1:3, nx, O, :], H.at[s, 1:3, 0, O, :]),
            (("+y",), hys.at[s], HY.at[s]),
            (("+z",), hzs.at[s], HP.at[s]),
        )
        steps, source, target = table[d]
        dev, can_send, can_recv = route(steps)
        return remote(source, target, h_send.at[s, d], h_recv.at[s, d], dev), can_send, can_recv

    def start(item, extra=None):
        copy, can_send, _ = item

        @pl.when(can_send if extra is None else can_send & extra)
        def _():
            copy.start()

    def finish(item):
        copy, can_send, _ = item

        @pl.when(can_send)
        def _():
            copy.wait_send()

    def arrive(item):
        copy, _, can_recv = item

        @pl.when(can_recv)
        def _():
            copy.wait_recv()

    def pack_column(acc, value, source, j):
        return jnp.where(lane == j, pltpu.roll(value, (j - source) % nz, 1), acc)

    def up_z(value, halo, j):
        return jnp.where(lane == nz - 1, pltpu.roll(halo, (nz - 1 - j) % nz, 1), pltpu.roll(value, nz - 1, 1))

    def down_z(value, halo, j):
        rolled = pltpu.roll(value, 1, 1)
        return jnp.where(lane == 0, pltpu.roll(halo, (nz - j) % nz, 1), rolled)

    def pack_rows(s, p, ex, ey, ez):
        ysU[s, 0, p : p + 1, :] = ex[ny - 1 : ny, :]
        ysU[s, 1, p : p + 1, :] = ey[ny - 1 : ny, :]
        ysU[s, 2, p : p + 1, :] = ez[ny - 1 : ny, :]
        ysD[s, 0, p : p + 1, :] = ex[0:1, :]
        ysD[s, 1, p : p + 1, :] = ez[0:1, :]
        if p == nx - 1:
            e1s[s] = ex[0:1, :]
        if p == 0:
            e2s[s] = ey[ny - 1 : ny, :]

    def pack_low(s):
        acc = jnp.zeros((ny, nz), F32)
        for p in range(nx):
            acc = pack_column(acc, E[s, 0, p, own, :], 0, p)
            acc = pack_column(acc, E[s, 1, p, own, :], 0, nx + p)
        zsD[s] = acc

    def pack_high(s):
        acc = jnp.zeros((ny, nz), F32)
        for p in range(nx):
            acc = pack_column(acc, E[s, 0, p, own, :], nz - 1, p)
            acc = pack_column(acc, E[s, 1, p, own, :], nz - 1, nx + p)
            acc = pack_column(acc, E[s, 2, p, own, :], nz - 1, 2 * nx + p)
        zsU[s] = acc

    def send_z(s, slot, extra=None):
        for sign, pack, d in (("-z", pack_low, 5), ("+z", pack_high, 4)):
            @pl.when(has[sign] if extra is None else has[sign] & extra)
            def _():
                pack(s)
                face(s, slot, d)[0].start()

    def send_first(s):
        for d in (8, 9, 0, 1):
            start(face(s, 0, d))
        for p in range(nx):
            pack_rows(s, p, E[s, 0, p, own, :], E[s, 1, p, own, :], E[s, 2, p, own, :])
        for d in (10, 11, 6, 7, 2, 3):
            start(face(s, 0, d))
        send_z(s, 0)

    def send_magnetic(s):
        start(first(s, 0))
        for p in range(nx):
            hys[s, 0, p : p + 1, :] = H[s, 0, p + 1, pad + ny - 1 : pad + ny, :]
            hys[s, 1, p : p + 1, :] = H[s, 2, p + 1, pad + ny - 1 : pad + ny, :]
        start(first(s, 1))

        @pl.when(has["+z"])
        def _():
            acc = jnp.zeros((ny, nz), F32)
            for p in range(nx):
                acc = pack_column(acc, H[s, 1, p + 1, O, :], nz - 1, p)
                acc = pack_column(acc, H[s, 0, p + 1, O, :], nz - 1, nx + p)
            hzs[s] = acc
            first(s, 2)[0].start()

    half_x = jnp.where(has["-x"], HALF, 0.0)
    half_y = jnp.where(has["-y"], HALF, 0.0)

    base = nx * ny
    rim = base + 2 * ny + 2 * nx

    def add_late(slot):
        for d in range(12):
            finish(face(1, slot, d))
        for p in range(nx):
            extra = late[p * ny : (p + 1) * ny, :]
            E[1, 2, p, own, :] = E[1, 2, p, own, :] + extra
            A[0, 2, p] = A[0, 2, p] + extra

    def update_h(s, slot, opening, behind=False):
        if behind:
            add_late(slot)
        for d in (3, 5):
            arrive(face(s, slot, d))
        for p in range(nx):
            E[s, 0, p, ny : ny + 1, :] = yD[slot, s, 0, p : p + 1, :]
            if behind:
                at = base + 2 * ny + nx + p
                E[s, 2, p, ny : ny + 1, :] = yD[slot, s, 1, p : p + 1, :] + late[at : at + 1, :]
            else:
                E[s, 2, p, ny : ny + 1, :] = yD[slot, s, 1, p : p + 1, :]
        halo = zD[slot, s]
        for p in range(nx):
            if p == nx - 1:
                for d in (0, 1):
                    arrive(face(s, slot, d))
                next_y, next_z = xD[slot, s, 0], xD[slot, s, 1]
                if behind:
                    next_z = next_z + late[base + ny : base + 2 * ny, :]
            else:
                next_y, next_z = E[s, 1, p + 1, own, :], E[s, 2, p + 1, own, :]
            ex, ey, ez = E[s, 0, p, own, :], E[s, 1, p, own, :], E[s, 2, p, own, :]
            hx = H[s, 0, p + 1, O, :] - HALF * (E[s, 2, p, above, :] - ez - (up_z(ey, halo, nx + p) - ey))
            hy = H[s, 1, p + 1, O, :] - HALF * (up_z(ex, halo, p) - ex - (next_z - ez))
            hz = H[s, 2, p + 1, O, :] - HALF * (next_y - ey - (E[s, 0, p, above, :] - ex))
            H[s, 0, p + 1, O, :] = hx
            H[s, 1, p + 1, O, :] = hy
            H[s, 2, p + 1, O, :] = hz
        for d in (2, 6, 7, 8, 10):
            arrive(face(s, slot, d))
        if opening:
            arrive(first(s, 0))
            arrive(first(s, 1))
        xU[slot, s, 0, ny : ny + 1, :] = e1r[slot, s]
        yU[slot, s, 1, nx : nx + 1, :] = e2r[slot, s]
        ex, ey, ez = xU[slot, s, 0, own, :], xU[slot, s, 1, own, :], xU[slot, s, 2, own, :]
        if behind:
            ez = ez + late[base : base + ny, :]
        side_y = H[s, 1, 0, O, :] - half_x * (up_z(ex, zX[slot, s], 0) - ex - (E[s, 2, 0, own, :] - ez))
        side_z = H[s, 2, 0, O, :] - half_x * (E[s, 1, 0, own, :] - ey - (xU[slot, s, 0, above, :] - ex))
        H[s, 1, 0, O, :] = side_y
        H[s, 2, 0, O, :] = side_z
        ex, ey, ez = yU[slot, s, 0, 0:nx, :], yU[slot, s, 1, 0:nx, :], yU[slot, s, 2, 0:nx, :]
        far = jnp.where(lane_p == nz - 1, pltpu.roll(yzU[slot, s], nz - 1, 1), pltpu.roll(ey, nz - 1, 1))
        near = ysD[s, 1]
        if behind:
            ez = ez + late[base + 2 * ny : base + 2 * ny + nx, :]
            near = near + late[rim : rim + nx, :]
        hx = HY[s, 0] - half_y * (near - ez - (far - ey))
        hz = HY[s, 1] - half_y * (yU[slot, s, 1, 1 : nx + 1, :] - ey - (ysD[s, 0] - ex))
        HY[s, 0] = hx
        HY[s, 1] = hz
        for p in range(nx):
            H[s, 0, p + 1, pad - 1 : pad, :] = hx[p : p + 1, :]
            H[s, 2, p + 1, pad - 1 : pad, :] = hz[p : p + 1, :]
        for d in (4, 9, 11):
            arrive(face(s, slot, d))
        if opening:
            arrive(first(s, 2))

        @pl.when(has["-z"])
        def _():
            edge, far_x = yzD[slot, s], zXU[slot, s]
            if behind:
                edge = edge + late_z[ny : ny + nx, :]
                far_x = far_x + late_z[0:ny, :]
                zU[slot, s, own, :] = zU[slot, s, own, :] + late_z[0:ny, :]
            edge = jnp.broadcast_to(edge[:, nz - 1 : nz], (nx, nz))
            edge = jnp.sum(jnp.where(lane_p == nx + row_p, edge, 0.0), axis=0, keepdims=True)
            below = zU[slot, s, own, :]
            next_i = jnp.where(lane == nx - 1, pltpu.roll(far_x, nx, 1), pltpu.roll(below, nz - 2 * nx - 1, 1))
            next_j = jnp.where(row == ny - 1, edge, pltpu.roll(zU[slot, s, above, :], nz - nx, 1))
            along = next_i - pltpu.roll(below, nz - 2 * nx, 1)
            across = next_j - pltpu.roll(below, nz - nx, 1)
            change = jnp.where(lane < nx, along, across)
            HP[s] = HP[s] - jnp.where(lane < nx, HALF, -HALF) * (zsD[s] - below - change)

    src = src_ref[0]
    total_z, total_y = nz * gz, ny * gy
    src_i = lax.div(src, total_y * total_z) - ix * nx
    src_j = lax.rem(lax.div(src, total_z), total_y) - iy * ny
    src_k = lax.rem(src, total_z) - iz * nz
    src_mask = (row == src_j) & (lane == src_k)

    def update_e(s, k, slot, behind=False):
        if not behind:
            for d in range(12):
                finish(face(s, slot, d))
        more = k < STEPS - 1
        halo = HP[s]
        below = slice(pad - 1, pad + ny - 1)
        pulse = wav_ref[begin + k]
        for p in (nx - 1,) + tuple(range(nx - 1)):
            hx, hy, hz = H[s, 0, p + 1, O, :], H[s, 1, p + 1, O, :], H[s, 2, p + 1, O, :]
            kp, cl = keep[p], curl[p]
            ox, oy, oz = E[s, 0, p, own, :], E[s, 1, p, own, :], E[s, 2, p, own, :]
            ex = kp * ox + cl * (hz - H[s, 2, p + 1, below, :] - (hy - down_z(hy, halo, p)))
            ey = kp * oy + cl * (hx - down_z(hx, halo, nx + p) - (hz - H[s, 2, p, O, :]))
            ez = kp * oz + cl * (hy - H[s, 1, p, O, :] - (hx - H[s, 0, p + 1, below, :]))
            if s == 0:
                ez = ez + jnp.where(src_mask, jnp.where(src_i == p, pulse, 0.0), 0.0)
                D[k, 0, p] = ex - ox
                D[k, 1, p] = ey - oy
                D[k, 2, p] = ez - oz
            else:
                if not (isinstance(k, int) and k == 0):
                    ez = ez + inj[k, p * ny : (p + 1) * ny, :]
                A[k, 0, p] = ex
                A[k, 1, p] = ey
                A[k, 2, p] = ez
            E[s, 0, p, own, :] = ex
            E[s, 1, p, own, :] = ey
            E[s, 2, p, own, :] = ez
            pack_rows(s, p, ex, ey, ez)
            if p == nx - 1:
                for d in (6, 8, 0):
                    start(face(s, 1 - slot, d), more)
            if p == 0:
                for d in (7, 9, 1):
                    start(face(s, 1 - slot, d), more)
        for d in (10, 11, 2, 3):
            start(face(s, 1 - slot, d), more)
        send_z(s, 1 - slot, more)

    count = cells_ref.shape[1]

    def place_cells():
        cells = cells_ref[...]
        i = lax.div(cells, total_y * total_z) - ix * nx
        j = lax.rem(lax.div(cells, total_z), total_y) - iy * ny
        k = lax.rem(cells, total_z) - iz * nz
        in_x, in_y = (i >= 0) & (i < nx), (j >= 0) & (j < ny)
        where = jnp.where(in_x & in_y, i * ny + j, -1)
        where = jnp.where((i == -1) & in_y, base + j, where)
        where = jnp.where((i == nx) & in_y, base + ny + j, where)
        where = jnp.where((j == -1) & in_x, base + 2 * ny + i, where)
        where = jnp.where((j == ny) & in_x, base + 2 * ny + nx + i, where)
        again = jnp.where((j == 0) & in_x, rim + i, -1)
        rows = lax.broadcasted_iota(jnp.int32, spots.shape, 0)
        spots[...] = jnp.where((rows == where) | (rows == again), 1.0, 0.0).astype(jnp.bfloat16)
        where = jnp.where(in_y & (i >= 0) & (i <= nx) & (k == -1), j, -1)
        where = jnp.where((j == ny) & in_x & (k == -1), ny + i, where)
        rows = lax.broadcasted_iota(jnp.int32, spots_z.shape, 0)
        spots_z[...] = jnp.where(rows == where, 1.0, 0.0).astype(jnp.bfloat16)

    nt = (((1,), (1,)), ((), ()))

    def sampled(m):
        spread_lane = lax.broadcasted_iota(jnp.int32, (nz, count), 0)
        spread_rec = lax.rem(lax.broadcasted_iota(jnp.int32, (nz, count), 1), per)
        device = lax.div(lax.broadcasted_iota(jnp.int32, (gy * nplane, count), 1), per)
        at_x, at_y, at_z = device // (gy * gz), lax.rem(device // gz, gy), lax.rem(device, gz)
        holder = at_y * nplane + at_x * gz + at_z == lax.broadcasted_iota(jnp.int32, (gy * nplane, count), 0)
        spread = jnp.where(spread_lane == m * per + spread_rec, 1.0, 0.0)
        found = jnp.dot(R_all[:, 0, :], spread, precision=lax.Precision.HIGHEST, preferred_element_type=F32)
        return jnp.sum(jnp.where(holder, found, 0.0), axis=0, keepdims=True)

    def spread_out(rows, rest):
        total = jnp.zeros((rows.shape[0], nz), F32)
        for _ in range(3):
            head = rest.astype(jnp.bfloat16)
            rest = rest - head.astype(F32)
            total = total + lax.dot_general(rows, head, nt, preferred_element_type=F32)
        return total

    lane_c = lax.broadcasted_iota(jnp.int32, (nz, count), 0)

    def inject(m):
        k = lax.rem(cells_ref[...], total_z) - iz * nz
        inj[m] = spread_out(spots[0:base, :], jnp.where(lane_c == k, sampled(m), 0.0))

    def inject_late():
        cells = cells_ref[...]
        k = lax.rem(cells, total_z) - iz * nz
        i = lax.div(cells, total_y * total_z) - ix * nx
        samples = sampled(0)
        late[...] = spread_out(spots[...], jnp.where(lane_c == k, samples, 0.0))
        j = lax.rem(lax.div(cells, total_z), total_y) - iy * ny
        at = jnp.where((i == nx) | (j == ny), nz - 1, 2 * nx + i)
        late_z[...] = spread_out(spots_z[...], jnp.where(lane_c == at, samples, 0.0))

    gather = exchange(layer, spot, mine.at[0], lambda q: R_all.at[iy * nplane + q], g_send, g_recv)
    for s in range(2):
        loads[s].wait()
        send_first(s)
        loads[2 + s].wait()
        send_magnetic(s)
    loads[4].wait()
    loads[5].wait()
    for p in range(nx):
        lo = loss[p]
        keep[p] = (1.0 - lo) / (1.0 + lo)
        curl[p] = 0.5 / (perm[p] * (1.0 + lo))
    for step in range(hops):
        pl.semaphore_wait(told.at[step], beside)
        if step < hops - 1:
            tell(step + 1)
    settle(gather)
    block = R_all.at[pl.ds(iy * nplane, nplane)]
    gather = exchange(line, iy, block, lambda q: R_all.at[pl.ds(q * nplane, nplane)], l_send, l_recv)
    place_cells()

    for s in range(2):
        for d in range(3):
            finish(first(s, d))
        update_h(s, 0, True)
    update_e(0, 0, 0)
    update_e(1, 0, 0)
    settle(gather)
    inject_late()
    inject(1)
    update_h(0, 1, False)
    update_e(0, 1, 1)
    update_h(1, 1, False, True)
    update_e(1, 1, 1, True)
    inject(2)

    def body(k, carry):
        slot = lax.rem(k, 2)
        for s in range(2):
            update_h(s, slot, False)
            update_e(s, k, slot)

        @pl.when(k < STEPS - 1)
        def _():
            inject(k + 1)

        return carry

    lax.fori_loop(2, STEPS, body, 0)

    squares = jnp.zeros((ny, nz), F32)
    for p in range(nx):
        total = jnp.zeros((ny, nz), F32)
        for m in range(STEPS):
            n = STEPS - 1 - m
            total = total + (D[n, 0, p] * A[m, 0, p] + D[n, 1, p] * A[m, 1, p] + D[n, 2, p] * A[m, 2, p])
        g = -total / perm[p]
        grad[p] = g
        squares = squares + g * g
    part[0] = jnp.sum(squares, axis=0, keepdims=True)
    devices = gy * nplane
    me = iy * nplane + spot
    peers = []
    for d in range(1, devices):
        q = lax.rem(me + d, devices)
        peers.append((q, (lax.rem(q // gz, gx), q // nplane, lax.rem(q, gz))))
    sums[pl.ds(me, 1)] = part[...]
    final = exchange(peers, me, part.at[0], lambda q: sums.at[q], r_send, r_recv)
    for _, recv in final:
        recv.wait_recv()
    tile = sums[:, 0, :]
    total = jnp.sum(jnp.sum(tile, axis=0, keepdims=True), axis=1, keepdims=True)
    rms = jnp.sqrt(total / (nx * ny * nz * gx * gy * gz) + 1e-06)
    rms_ref[...] = rms
    inverse = 1.0 / rms
    for p in range(nx):
        out_ref[p] = grad[p] * inverse
    for send, _ in final:
        send.wait_send()


def per_device(
    permittivity, loss, fwd_electric, fwd_magnetic, adj_electric, adj_magnetic,
    wavelet, residuals, source_cell, receiver_cells, start_step,
):
    sizes = tuple(lax.axis_size(a) for a in ("gx", "gy", "gz"))
    gx, gy, gz = sizes
    nx, ny, nz = permittivity.shape
    devices = gx * gy * gz
    count = receiver_cells.shape[0]
    vmem = pl.BlockSpec(memory_space=pltpu.VMEM)
    hbm = pl.BlockSpec(memory_space=pltpu.HBM)
    dma = pltpu.SemaphoreType.DMA
    block = (nx, ny, nz)

    extended = -(-(nx * ny + 2 * ny + 3 * nx) // 16) * 16
    flat = -(-(ny + nx) // 16) * 16

    def room(*shape):
        return pltpu.VMEM(shape, F32)

    direction, rms = pl.pallas_call(
        functools.partial(kernel, sizes),
        out_shape=(
            pltpu.VMEM(block, F32),
            jax.ShapeDtypeStruct((1, 1), F32),
        ),
        in_specs=[hbm] * 11,
        out_specs=(vmem, vmem),
        scratch_shapes=[
            room(2, 3, nx, ny + 8, nz),
            room(2, 3, nx + 1, ny + 8, nz),
            room(*block),
            room(*block),
            room(*block),
            room(*block),
            room(STEPS, 3, *block),
            room(STEPS, 3, *block),
            room(STEPS, nx * ny, nz),
            room(extended, nz),
            room(flat, nz),
            pltpu.VMEM((extended, count), jnp.bfloat16),
            pltpu.VMEM((flat, count), jnp.bfloat16),
            room(devices, 1, nz),
            room(*block),
            room(2, 2, nx, nz),
            room(2, ny, nz),
            room(2, 2, 3, ny + 8, nz),
            room(2, 2, 2, ny, nz),
            room(2, 3, nx, nz),
            room(2, 2, nx, nz),
            room(2, 2, 3, nx + 8, nz),
            room(2, 2, 2, nx, nz),
            room(2, 2, nx, nz),
            room(2, 2, nx, nz),
            room(2, ny, nz),
            room(2, ny, nz),
            room(2, 2, ny + 8, nz),
            room(2, 2, ny, nz),
            room(2, 2, ny, nz),
            room(2, 2, ny, nz),
            room(2, 1, nz),
            room(2, 1, nz),
            room(2, 2, 1, nz),
            room(2, 2, 1, nz),
            room(2, 2, nx, nz),
            room(2, ny, nz),
            room(1, 1, nz),
            room(devices, 1, nz),
            pltpu.SMEM(wavelet.shape, F32),
            pltpu.SMEM((1,), jnp.int32),
            pltpu.SMEM((1,), jnp.int32),
            pltpu.VMEM((1, count), jnp.int32),
            room(*residuals.shape),
            room(1, 1, nz),
            dma((11,)),
            dma((2, 12)),
            dma((2, 2, 12)),
            dma((2, 3)),
            dma((2, 3)),
            dma((gx * gz,)),
            dma((gx * gz,)),
            dma((gy,)),
            dma((gy,)),
            pltpu.SemaphoreType.REGULAR((max(gy - 2, 1),)),
            dma((devices,)),
            dma((devices,)),
        ],
        compiler_params=pltpu.CompilerParams(
            collective_id=0, has_side_effects=True, vmem_limit_bytes=60 * 1024 * 1024
        ),
    )(
        wavelet, source_cell, start_step, receiver_cells.reshape(1, count),
        permittivity, loss, fwd_electric, fwd_magnetic, adj_electric, adj_magnetic, residuals,
    )
    return direction, rms.reshape(())


def solution(mesh):
    block = P("gx", "gy", "gz")
    state = P(None, "gx", "gy", "gz")
    return jax.shard_map(
        per_device,
        mesh=mesh,
        in_specs=(
            block, block, state, state, state, state,
            P(), P(("gx", "gy", "gz"), None), P(), P(), P(),
        ),
        out_specs=(block, P()),
        check_vma=False,
    )
```

```python
import functools

import jax
import jax.numpy as jnp
from jax import lax
from jax.experimental import pallas as pl
from jax.experimental.pallas import tpu as pltpu
from jax.sharding import PartitionSpec as P

STEPS = 4
MESH = pl.DeviceIdType.MESH
F32 = jnp.float32
HALF = 0.5


def kernel(
    sizes,
    wav_hbm,
    src_hbm,
    start_hbm,
    cells_hbm,
    perm_hbm,
    loss_hbm,
    fe_hbm,
    fm_hbm,
    ae_hbm,
    am_hbm,
    res_hbm,
    out_ref,
    rms_ref,
    E,
    H,
    perm,
    loss,
    keep,
    curl,
    D,
    A,
    inj,
    late,
    late_z,
    spots,
    spots_z,
    R_all,
    grad,
    HY,
    HP,
    xU,
    xD,
    ysU,
    ysD,
    yU,
    yD,
    yzU,
    yzD,
    zsU,
    zsD,
    zU,
    zD,
    zX,
    zXU,
    e1s,
    e2s,
    e1r,
    e2r,
    hys,
    hzs,
    part,
    sums,
    wav_ref,
    src_ref,
    start_ref,
    cells_ref,
    res_ref,
    mine,
    load_sem,
    f_send,
    f_recv,
    h_send,
    h_recv,
    g_send,
    g_recv,
    l_send,
    l_recv,
    told,
    r_send,
    r_recv,
):
    gx, gy, gz = sizes
    nx, ny, nz = perm.shape
    pad = H.shape[3] - ny
    own = slice(0, ny)
    above = slice(1, ny + 1)
    O = slice(pad, pad + ny)
    ix, iy, iz = lax.axis_index("gx"), lax.axis_index("gy"), lax.axis_index("gz")
    nplane = gx * gz
    spot = ix * gz + iz

    loads = [
        pltpu.make_async_copy(fe_hbm, E.at[0, :, :, own, :], load_sem.at[0]),
        pltpu.make_async_copy(ae_hbm, E.at[1, :, :, own, :], load_sem.at[1]),
        pltpu.make_async_copy(fm_hbm, H.at[0, :, 1 : nx + 1, O, :], load_sem.at[2]),
        pltpu.make_async_copy(am_hbm, H.at[1, :, 1 : nx + 1, O, :], load_sem.at[3]),
        pltpu.make_async_copy(loss_hbm, loss, load_sem.at[4]),
        pltpu.make_async_copy(perm_hbm, perm, load_sem.at[5]),
    ]
    small = [
        pltpu.make_async_copy(start_hbm, start_ref, load_sem.at[6]),
        pltpu.make_async_copy(res_hbm, res_ref, load_sem.at[7]),
        pltpu.make_async_copy(src_hbm, src_ref, load_sem.at[8]),
        pltpu.make_async_copy(wav_hbm, wav_ref, load_sem.at[9]),
        pltpu.make_async_copy(cells_hbm, cells_ref, load_sem.at[10]),
    ]
    for load in small:
        load.start()
    for i in (0, 2, 1, 3, 4, 5):
        loads[i].start()

    zero_plane = jnp.zeros((ny, nz), F32)
    zero_row = jnp.zeros((1, nz), F32)
    for s in range(2):
        for c in range(3):
            for p in range(nx):
                E[s, c, p, ny : ny + 1, :] = zero_row
        for c in (1, 2):
            H[s, c, 0, O, :] = zero_plane
    for buffer in (HY, HP, xU, xD, yU, yD, yzU, yzD, zU, zD, zX, zXU, e1r, e2r):
        buffer[...] = jnp.zeros(buffer.shape, F32)

    has = {
        "+x": ix < gx - 1, "-x": ix > 0, "+y": iy < gy - 1,
        "-y": iy > 0, "+z": iz < gz - 1, "-z": iz > 0,
    }
    flip = {"+": "-", "-": "+"}

    def route(steps):
        dev = [ix, iy, iz]
        size = (gx, gy, gz)
        can_send, can_recv = True, True
        for step in steps:
            axis = "xyz".index(step[1])
            dev[axis] = jnp.clip(dev[axis] + (1 if step[0] == "+" else -1), 0, size[axis] - 1)
            back = flip[step[0]] + step[1]
            can_send = has[step] if can_send is True else can_send & has[step]
            can_recv = has[back] if can_recv is True else can_recv & has[back]
        return tuple(dev), can_send, can_recv

    layer = []
    for d in range(1, nplane):
        q = lax.rem(spot + d, nplane)
        layer.append((q, (q // gz, iy, lax.rem(q, gz))))
    line = []
    for d in range(1, gy):
        q = lax.rem(iy + d, gy)
        line.append((q, (ix, q, iz)))
    barrier = pltpu.get_barrier_semaphore()
    greeted = len(layer)
    beside = has["+y"].astype(jnp.int32) + has["-y"].astype(jnp.int32)
    for steps in (("+y",), ("-y",), ("+x", "-y"), ("-x", "+y"), ("+y", "-z"), ("-y", "+z")):
        dev, can_send, _ = route(steps)
        greeted = greeted + can_send.astype(jnp.int32)

        @pl.when(can_send)
        def _():
            pl.semaphore_signal(barrier, inc=1, device_id=dev, device_id_type=MESH)

    for _, dev in layer:
        pl.semaphore_signal(barrier, inc=1, device_id=dev, device_id_type=MESH)

    lane = lax.broadcasted_iota(jnp.int32, (ny, nz), 1)
    row = lax.broadcasted_iota(jnp.int32, (ny, nz), 0)
    lane_p = lax.broadcasted_iota(jnp.int32, (nx, nz), 1)
    row_p = lax.broadcasted_iota(jnp.int32, (nx, nz), 0)

    per, trace = res_hbm.shape
    small[0].wait()
    small[1].wait()
    begin = start_ref[0]
    time_at = lax.broadcasted_iota(jnp.int32, (trace, nz), 0)
    turn = lax.div(lax.broadcasted_iota(jnp.int32, (trace, nz), 1), per)
    pick = jnp.where(time_at == begin + STEPS - 1 - turn, 1.0, 0.0)
    found = jnp.dot(res_ref[...], pick, precision=lax.Precision.HIGHEST, preferred_element_type=F32)
    mask = lax.rem(lax.broadcasted_iota(jnp.int32, (per, nz), 1), per)
    mask = mask == lax.broadcasted_iota(jnp.int32, (per, nz), 0)
    mine[0] = jnp.sum(jnp.where(mask, found, 0.0), axis=0, keepdims=True)
    R_all[pl.ds(iy * nplane + spot, 1)] = mine[...]
    for load in small[2:]:
        load.wait()
    pl.semaphore_wait(barrier, greeted)

    def tell(step):
        for way in ("+y", "-y"):
            dev, can_send, _ = route((way,))

            @pl.when(can_send)
            def _():
                pl.semaphore_signal(told.at[step], inc=1, device_id=dev, device_id_type=MESH)

    hops = gy - 2
    if hops > 0:
        tell(0)

    def remote(src, dst, ssem, rsem, dev):
        return pltpu.make_async_remote_copy(
            src_ref=src, dst_ref=dst, send_sem=ssem, recv_sem=rsem,
            device_id=dev, device_id_type=MESH,
        )

    def exchange(peers, at, src, slots, send_sems, recv_sems):
        copies = []
        for d, (q, dev) in enumerate(peers):
            send = remote(src, slots(at), send_sems.at[d], recv_sems.at[at], dev)
            recv = remote(src, slots(q), send_sems.at[d], recv_sems.at[q], dev)
            send.start()
            copies.append((send, recv))
        return copies

    def settle(copies):
        for send, recv in copies:
            recv.wait_recv()
        for send, recv in copies:
            send.wait_send()

    def face(s, slot, d):
        table = (
            (("+x",), E.at[s, :, nx - 1, own, :], xU.at[slot, s, :, own, :]),
            (("-x",), E.at[s, 1:3, 0, own, :], xD.at[slot, s]),
            (("+y",), ysU.at[s], yU.at[slot, s, :, 0:nx, :]),
            (("-y",), ysD.at[s], yD.at[slot, s]),
            (("+z",), zsU.at[s], zU.at[slot, s, own, :]),
            (("-z",), zsD.at[s], zD.at[slot, s]),
            (("+x", "-y"), e1s.at[s], e1r.at[slot, s]),
            (("-x", "+y"), e2s.at[s], e2r.at[slot, s]),
            (("+x", "-z"), E.at[s, 0, nx - 1, own, :], zX.at[slot, s]),
            (("-x", "+z"), E.at[s, 2, 0, own, :], zXU.at[slot, s]),
            (("+y", "-z"), ysU.at[s, 1], yzU.at[slot, s]),
            (("-y", "+z"), ysD.at[s, 1], yzD.at[slot, s]),
        )
        steps, source, target = table[d]
        dev, can_send, can_recv = route(steps)
        return remote(source, target, f_send.at[s, d], f_recv.at[slot, s, d], dev), can_send, can_recv

    def first(s, d):
        table = (
            (("+x",), H.at[s, 1:3, nx, O, :], H.at[s, 1:3, 0, O, :]),
            (("+y",), hys.at[s], HY.at[s]),
            (("+z",), hzs.at[s], HP.at[s]),
        )
        steps, source, target = table[d]
        dev, can_send, can_recv = route(steps)
        return remote(source, target, h_send.at[s, d], h_recv.at[s, d], dev), can_send, can_recv

    def start(item, extra=None):
        copy, can_send, _ = item

        @pl.when(can_send if extra is None else can_send & extra)
        def _():
            copy.start()

    def finish(item):
        copy, can_send, _ = item

        @pl.when(can_send)
        def _():
            copy.wait_send()

    def arrive(item):
        copy, _, can_recv = item

        @pl.when(can_recv)
        def _():
            copy.wait_recv()

    def pack_column(acc, value, source, j):
        return jnp.where(lane == j, pltpu.roll(value, (j - source) % nz, 1), acc)

    def up_z(value, halo, j):
        return jnp.where(lane == nz - 1, pltpu.roll(halo, (nz - 1 - j) % nz, 1), pltpu.roll(value, nz - 1, 1))

    def down_z(value, halo, j):
        rolled = pltpu.roll(value, 1, 1)
        return jnp.where(lane == 0, pltpu.roll(halo, (nz - j) % nz, 1), rolled)

    def pack_rows(s, p, ex, ey, ez):
        ysU[s, 0, p : p + 1, :] = ex[ny - 1 : ny, :]
        ysU[s, 1, p : p + 1, :] = ey[ny - 1 : ny, :]
        ysU[s, 2, p : p + 1, :] = ez[ny - 1 : ny, :]
        ysD[s, 0, p : p + 1, :] = ex[0:1, :]
        ysD[s, 1, p : p + 1, :] = ez[0:1, :]
        if p == nx - 1:
            e1s[s] = ex[0:1, :]
        if p == 0:
            e2s[s] = ey[ny - 1 : ny, :]

    def pack_low(s):
        acc = jnp.zeros((ny, nz), F32)
        for p in range(nx):
            acc = pack_column(acc, E[s, 0, p, own, :], 0, p)
            acc = pack_column(acc, E[s, 1, p, own, :], 0, nx + p)
        zsD[s] = acc

    def pack_high(s):
        acc = jnp.zeros((ny, nz), F32)
        for p in range(nx):
            acc = pack_column(acc, E[s, 0, p, own, :], nz - 1, p)
            acc = pack_column(acc, E[s, 1, p, own, :], nz - 1, nx + p)
            acc = pack_column(acc, E[s, 2, p, own, :], nz - 1, 2 * nx + p)
        zsU[s] = acc

    def send_z(s, slot, extra=None):
        for sign, pack, d in (("-z", pack_low, 5), ("+z", pack_high, 4)):
            @pl.when(has[sign] if extra is None else has[sign] & extra)
            def _():
                pack(s)
                face(s, slot, d)[0].start()

    def send_first(s):
        for d in (8, 9, 0, 1):
            start(face(s, 0, d))
        for p in range(nx):
            pack_rows(s, p, E[s, 0, p, own, :], E[s, 1, p, own, :], E[s, 2, p, own, :])
        for d in (10, 11, 6, 7, 2, 3):
            start(face(s, 0, d))
        send_z(s, 0)

    def send_magnetic(s):
        start(first(s, 0))
        for p in range(nx):
            hys[s, 0, p : p + 1, :] = H[s, 0, p + 1, pad + ny - 1 : pad + ny, :]
            hys[s, 1, p : p + 1, :] = H[s, 2, p + 1, pad + ny - 1 : pad + ny, :]
        start(first(s, 1))

        @pl.when(has["+z"])
        def _():
            acc = jnp.zeros((ny, nz), F32)
            for p in range(nx):
                acc = pack_column(acc, H[s, 1, p + 1, O, :], nz - 1, p)
                acc = pack_column(acc, H[s, 0, p + 1, O, :], nz - 1, nx + p)
            hzs[s] = acc
            first(s, 2)[0].start()

    half_x = jnp.where(has["-x"], HALF, 0.0)
    half_y = jnp.where(has["-y"], HALF, 0.0)

    base = nx * ny
    rim = base + 2 * ny + 2 * nx

    def add_late(slot):
        for d in range(12):
            finish(face(1, slot, d))
        for p in range(nx):
            extra = late[p * ny : (p + 1) * ny, :]
            E[1, 2, p, own, :] = E[1, 2, p, own, :] + extra
            A[0, 2, p] = A[0, 2, p] + extra

    def update_h(s, slot, opening, behind=False):
        if behind:
            add_late(slot)
        for d in (3, 5):
            arrive(face(s, slot, d))
        for p in range(nx):
            E[s, 0, p, ny : ny + 1, :] = yD[slot, s, 0, p : p + 1, :]
            if behind:
                at = base + 2 * ny + nx + p
                E[s, 2, p, ny : ny + 1, :] = yD[slot, s, 1, p : p + 1, :] + late[at : at + 1, :]
            else:
                E[s, 2, p, ny : ny + 1, :] = yD[slot, s, 1, p : p + 1, :]
        halo = zD[slot, s]
        for p in range(nx):
            if p == nx - 1:
                for d in (0, 1):
                    arrive(face(s, slot, d))
                next_y, next_z = xD[slot, s, 0], xD[slot, s, 1]
                if behind:
                    next_z = next_z + late[base + ny : base + 2 * ny, :]
            else:
                next_y, next_z = E[s, 1, p + 1, own, :], E[s, 2, p + 1, own, :]
            ex, ey, ez = E[s, 0, p, own, :], E[s, 1, p, own, :], E[s, 2, p, own, :]
            hx = H[s, 0, p + 1, O, :] - HALF * (E[s, 2, p, above, :] - ez - (up_z(ey, halo, nx + p) - ey))
            hy = H[s, 1, p + 1, O, :] - HALF * (up_z(ex, halo, p) - ex - (next_z - ez))
            hz = H[s, 2, p + 1, O, :] - HALF * (next_y - ey - (E[s, 0, p, above, :] - ex))
            H[s, 0, p + 1, O, :] = hx
            H[s, 1, p + 1, O, :] = hy
            H[s, 2, p + 1, O, :] = hz
        for d in (2, 6, 7, 8, 10):
            arrive(face(s, slot, d))
        if opening:
            arrive(first(s, 0))
            arrive(first(s, 1))
        xU[slot, s, 0, ny : ny + 1, :] = e1r[slot, s]
        yU[slot, s, 1, nx : nx + 1, :] = e2r[slot, s]
        ex, ey, ez = xU[slot, s, 0, own, :], xU[slot, s, 1, own, :], xU[slot, s, 2, own, :]
        if behind:
            ez = ez + late[base : base + ny, :]
        side_y = H[s, 1, 0, O, :] - half_x * (up_z(ex, zX[slot, s], 0) - ex - (E[s, 2, 0, own, :] - ez))
        side_z = H[s, 2, 0, O, :] - half_x * (E[s, 1, 0, own, :] - ey - (xU[slot, s, 0, above, :] - ex))
        H[s, 1, 0, O, :] = side_y
        H[s, 2, 0, O, :] = side_z
        ex, ey, ez = yU[slot, s, 0, 0:nx, :], yU[slot, s, 1, 0:nx, :], yU[slot, s, 2, 0:nx, :]
        far = jnp.where(lane_p == nz - 1, pltpu.roll(yzU[slot, s], nz - 1, 1), pltpu.roll(ey, nz - 1, 1))
        near = ysD[s, 1]
        if behind:
            ez = ez + late[base + 2 * ny : base + 2 * ny + nx, :]
            near = near + late[rim : rim + nx, :]
        hx = HY[s, 0] - half_y * (near - ez - (far - ey))
        hz = HY[s, 1] - half_y * (yU[slot, s, 1, 1 : nx + 1, :] - ey - (ysD[s, 0] - ex))
        HY[s, 0] = hx
        HY[s, 1] = hz
        for p in range(nx):
            H[s, 0, p + 1, pad - 1 : pad, :] = hx[p : p + 1, :]
            H[s, 2, p + 1, pad - 1 : pad, :] = hz[p : p + 1, :]
        for d in (4, 9, 11):
            arrive(face(s, slot, d))
        if opening:
            arrive(first(s, 2))

        @pl.when(has["-z"])
        def _():
            edge, far_x = yzD[slot, s], zXU[slot, s]
            if behind:
                edge = edge + late_z[ny : ny + nx, :]
                far_x = far_x + late_z[0:ny, :]
                zU[slot, s, own, :] = zU[slot, s, own, :] + late_z[0:ny, :]
            edge = jnp.broadcast_to(edge[:, nz - 1 : nz], (nx, nz))
            edge = jnp.sum(jnp.where(lane_p == nx + row_p, edge, 0.0), axis=0, keepdims=True)
            below = zU[slot, s, own, :]
            next_i = jnp.where(lane == nx - 1, pltpu.roll(far_x, nx, 1), pltpu.roll(below, nz - 2 * nx - 1, 1))
            next_j = jnp.where(row == ny - 1, edge, pltpu.roll(zU[slot, s, above, :], nz - nx, 1))
            along = next_i - pltpu.roll(below, nz - 2 * nx, 1)
            across = next_j - pltpu.roll(below, nz - nx, 1)
            change = jnp.where(lane < nx, along, across)
            HP[s] = HP[s] - jnp.where(lane < nx, HALF, -HALF) * (zsD[s] - below - change)

    src = src_ref[0]
    total_z, total_y = nz * gz, ny * gy
    src_i = lax.div(src, total_y * total_z) - ix * nx
    src_j = lax.rem(lax.div(src, total_z), total_y) - iy * ny
    src_k = lax.rem(src, total_z) - iz * nz
    src_mask = (row == src_j) & (lane == src_k)

    def update_e(s, k, slot, behind=False):
        if not behind:
            for d in range(12):
                finish(face(s, slot, d))
        more = k < STEPS - 1
        halo = HP[s]
        below = slice(pad - 1, pad + ny - 1)
        pulse = wav_ref[begin + k]
        for p in (nx - 1,) + tuple(range(nx - 1)):
            hx, hy, hz = H[s, 0, p + 1, O, :], H[s, 1, p + 1, O, :], H[s, 2, p + 1, O, :]
            kp, cl = keep[p], curl[p]
            ox, oy, oz = E[s, 0, p, own, :], E[s, 1, p, own, :], E[s, 2, p, own, :]
            ex = kp * ox + cl * (hz - H[s, 2, p + 1, below, :] - (hy - down_z(hy, halo, p)))
            ey = kp * oy + cl * (hx - down_z(hx, halo, nx + p) - (hz - H[s, 2, p, O, :]))
            ez = kp * oz + cl * (hy - H[s, 1, p, O, :] - (hx - H[s, 0, p + 1, below, :]))
            if s == 0:
                ez = ez + jnp.where(src_mask, jnp.where(src_i == p, pulse, 0.0), 0.0)
                D[k, 0, p] = ex - ox
                D[k, 1, p] = ey - oy
                D[k, 2, p] = ez - oz
            else:
                if not (isinstance(k, int) and k == 0):
                    ez = ez + inj[k, p * ny : (p + 1) * ny, :]
                A[k, 0, p] = ex
                A[k, 1, p] = ey
                A[k, 2, p] = ez
            E[s, 0, p, own, :] = ex
            E[s, 1, p, own, :] = ey
            E[s, 2, p, own, :] = ez
            pack_rows(s, p, ex, ey, ez)
            if p == nx - 1:
                for d in (6, 8, 0):
                    start(face(s, 1 - slot, d), more)
            if p == 0:
                for d in (7, 9, 1):
                    start(face(s, 1 - slot, d), more)
        for d in (10, 11, 2, 3):
            start(face(s, 1 - slot, d), more)
        send_z(s, 1 - slot, more)

    count = cells_ref.shape[1]

    def place_cells():
        cells = cells_ref[...]
        i = lax.div(cells, total_y * total_z) - ix * nx
        j = lax.rem(lax.div(cells, total_z), total_y) - iy * ny
        k = lax.rem(cells, total_z) - iz * nz
        in_x, in_y = (i >= 0) & (i < nx), (j >= 0) & (j < ny)
        where = jnp.where(in_x & in_y, i * ny + j, -1)
        where = jnp.where((i == -1) & in_y, base + j, where)
        where = jnp.where((i == nx) & in_y, base + ny + j, where)
        where = jnp.where((j == -1) & in_x, base + 2 * ny + i, where)
        where = jnp.where((j == ny) & in_x, base + 2 * ny + nx + i, where)
        again = jnp.where((j == 0) & in_x, rim + i, -1)
        rows = lax.broadcasted_iota(jnp.int32, spots.shape, 0)
        spots[...] = jnp.where((rows == where) | (rows == again), 1.0, 0.0).astype(jnp.bfloat16)
        where = jnp.where(in_y & (i >= 0) & (i <= nx) & (k == -1), j, -1)
        where = jnp.where((j == ny) & in_x & (k == -1), ny + i, where)
        rows = lax.broadcasted_iota(jnp.int32, spots_z.shape, 0)
        spots_z[...] = jnp.where(rows == where, 1.0, 0.0).astype(jnp.bfloat16)

    nt = (((1,), (1,)), ((), ()))

    def sampled(m):
        spread_lane = lax.broadcasted_iota(jnp.int32, (nz, count), 0)
        spread_rec = lax.rem(lax.broadcasted_iota(jnp.int32, (nz, count), 1), per)
        device = lax.div(lax.broadcasted_iota(jnp.int32, (gy * nplane, count), 1), per)
        at_x, at_y, at_z = device // (gy * gz), lax.rem(device // gz, gy), lax.rem(device, gz)
        holder = at_y * nplane + at_x * gz + at_z == lax.broadcasted_iota(jnp.int32, (gy * nplane, count), 0)
        spread = jnp.where(spread_lane == m * per + spread_rec, 1.0, 0.0)
        found = jnp.dot(R_all[:, 0, :], spread, precision=lax.Precision.HIGHEST, preferred_element_type=F32)
        return jnp.sum(jnp.where(holder, found, 0.0), axis=0, keepdims=True)

    def spread_out(rows, rest):
        total = jnp.zeros((rows.shape[0], nz), F32)
        for _ in range(3):
            head = rest.astype(jnp.bfloat16)
            rest = rest - head.astype(F32)
            total = total + lax.dot_general(rows, head, nt, preferred_element_type=F32)
        return total

    lane_c = lax.broadcasted_iota(jnp.int32, (nz, count), 0)

    def inject(m):
        k = lax.rem(cells_ref[...], total_z) - iz * nz
        inj[m] = spread_out(spots[0:base, :], jnp.where(lane_c == k, sampled(m), 0.0))

    def inject_late():
        cells = cells_ref[...]
        k = lax.rem(cells, total_z) - iz * nz
        i = lax.div(cells, total_y * total_z) - ix * nx
        samples = sampled(0)
        late[...] = spread_out(spots[...], jnp.where(lane_c == k, samples, 0.0))
        j = lax.rem(lax.div(cells, total_z), total_y) - iy * ny
        at = jnp.where((i == nx) | (j == ny), nz - 1, 2 * nx + i)
        late_z[...] = spread_out(spots_z[...], jnp.where(lane_c == at, samples, 0.0))

    gather = exchange(layer, spot, mine.at[0], lambda q: R_all.at[iy * nplane + q], g_send, g_recv)
    for s in range(2):
        loads[s].wait()
        send_first(s)
        loads[2 + s].wait()
        send_magnetic(s)
    loads[4].wait()
    loads[5].wait()
    for p in range(nx):
        lo = loss[p]
        keep[p] = (1.0 - lo) / (1.0 + lo)
        curl[p] = 0.5 / (perm[p] * (1.0 + lo))
    for step in range(hops):
        pl.semaphore_wait(told.at[step], beside)
        if step < hops - 1:
            tell(step + 1)
    settle(gather)
    block = R_all.at[pl.ds(iy * nplane, nplane)]
    gather = exchange(line, iy, block, lambda q: R_all.at[pl.ds(q * nplane, nplane)], l_send, l_recv)
    place_cells()

    for s in range(2):
        for d in range(3):
            finish(first(s, d))
        update_h(s, 0, True)
    update_e(0, 0, 0)
    update_e(1, 0, 0)
    update_h(0, 1, False)
    update_e(0, 1, 1)
    settle(gather)
    inject_late()
    inject(1)
    update_h(1, 1, False, True)
    update_e(1, 1, 1, True)
    inject(2)

    def body(k, carry):
        slot = lax.rem(k, 2)
        for s in range(2):
            update_h(s, slot, False)
            update_e(s, k, slot)

        @pl.when(k < STEPS - 1)
        def _():
            inject(k + 1)

        return carry

    lax.fori_loop(2, STEPS, body, 0)

    squares = jnp.zeros((ny, nz), F32)
    for p in range(nx):
        total = jnp.zeros((ny, nz), F32)
        for m in range(STEPS):
            n = STEPS - 1 - m
            total = total + (D[n, 0, p] * A[m, 0, p] + D[n, 1, p] * A[m, 1, p] + D[n, 2, p] * A[m, 2, p])
        g = -total / perm[p]
        grad[p] = g
        squares = squares + g * g
    part[0] = jnp.sum(squares, axis=0, keepdims=True)
    devices = gy * nplane
    me = iy * nplane + spot
    peers = []
    for d in range(1, devices):
        q = lax.rem(me + d, devices)
        peers.append((q, (lax.rem(q // gz, gx), q // nplane, lax.rem(q, gz))))
    sums[pl.ds(me, 1)] = part[...]
    final = exchange(peers, me, part.at[0], lambda q: sums.at[q], r_send, r_recv)
    for _, recv in final:
        recv.wait_recv()
    tile = sums[:, 0, :]
    total = jnp.sum(jnp.sum(tile, axis=0, keepdims=True), axis=1, keepdims=True)
    rms = jnp.sqrt(total / (nx * ny * nz * gx * gy * gz) + 1e-06)
    rms_ref[...] = rms
    inverse = 1.0 / rms
    for p in range(nx):
        out_ref[p] = grad[p] * inverse
    for send, _ in final:
        send.wait_send()


def per_device(
    permittivity, loss, fwd_electric, fwd_magnetic, adj_electric, adj_magnetic,
    wavelet, residuals, source_cell, receiver_cells, start_step,
):
    sizes = tuple(lax.axis_size(a) for a in ("gx", "gy", "gz"))
    gx, gy, gz = sizes
    nx, ny, nz = permittivity.shape
    devices = gx * gy * gz
    count = receiver_cells.shape[0]
    vmem = pl.BlockSpec(memory_space=pltpu.VMEM)
    hbm = pl.BlockSpec(memory_space=pltpu.HBM)
    dma = pltpu.SemaphoreType.DMA
    block = (nx, ny, nz)

    extended = -(-(nx * ny + 2 * ny + 3 * nx) // 16) * 16
    flat = -(-(ny + nx) // 16) * 16

    def room(*shape):
        return pltpu.VMEM(shape, F32)

    direction, rms = pl.pallas_call(
        functools.partial(kernel, sizes),
        out_shape=(
            pltpu.VMEM(block, F32),
            jax.ShapeDtypeStruct((1, 1), F32),
        ),
        in_specs=[hbm] * 11,
        out_specs=(vmem, vmem),
        scratch_shapes=[
            room(2, 3, nx, ny + 8, nz),
            room(2, 3, nx + 1, ny + 8, nz),
            room(*block),
            room(*block),
            room(*block),
            room(*block),
            room(STEPS, 3, *block),
            room(STEPS, 3, *block),
            room(STEPS, nx * ny, nz),
            room(extended, nz),
            room(flat, nz),
            pltpu.VMEM((extended, count), jnp.bfloat16),
            pltpu.VMEM((flat, count), jnp.bfloat16),
            room(devices, 1, nz),
            room(*block),
            room(2, 2, nx, nz),
            room(2, ny, nz),
            room(2, 2, 3, ny + 8, nz),
            room(2, 2, 2, ny, nz),
            room(2, 3, nx, nz),
            room(2, 2, nx, nz),
            room(2, 2, 3, nx + 8, nz),
            room(2, 2, 2, nx, nz),
            room(2, 2, nx, nz),
            room(2, 2, nx, nz),
            room(2, ny, nz),
            room(2, ny, nz),
            room(2, 2, ny + 8, nz),
            room(2, 2, ny, nz),
            room(2, 2, ny, nz),
            room(2, 2, ny, nz),
            room(2, 1, nz),
            room(2, 1, nz),
            room(2, 2, 1, nz),
            room(2, 2, 1, nz),
            room(2, 2, nx, nz),
            room(2, ny, nz),
            room(1, 1, nz),
            room(devices, 1, nz),
            pltpu.SMEM(wavelet.shape, F32),
            pltpu.SMEM((1,), jnp.int32),
            pltpu.SMEM((1,), jnp.int32),
            pltpu.VMEM((1, count), jnp.int32),
            room(*residuals.shape),
            room(1, 1, nz),
            dma((11,)),
            dma((2, 12)),
            dma((2, 2, 12)),
            dma((2, 3)),
            dma((2, 3)),
            dma((gx * gz,)),
            dma((gx * gz,)),
            dma((gy,)),
            dma((gy,)),
            pltpu.SemaphoreType.REGULAR((max(gy - 2, 1),)),
            dma((devices,)),
            dma((devices,)),
        ],
        compiler_params=pltpu.CompilerParams(
            collective_id=0, has_side_effects=True, vmem_limit_bytes=60 * 1024 * 1024
        ),
    )(
        wavelet, source_cell, start_step, receiver_cells.reshape(1, count),
        permittivity, loss, fwd_electric, fwd_magnetic, adj_electric, adj_magnetic, residuals,
    )
    return direction, rms.reshape(())


def solution(mesh):
    block = P("gx", "gy", "gz")
    state = P(None, "gx", "gy", "gz")
    return jax.shard_map(
        per_device,
        mesh=mesh,
        in_specs=(
            block, block, state, state, state, state,
            P(), P(("gx", "gy", "gz"), None), P(), P(), P(),
        ),
        out_specs=(block, P()),
        check_vma=False,
    )
```
